256 devices in a mesh: dp: 64 (over z, x, core), rank: 4 (over y).
Axes of the slice: x: 4, y: 4, z: 8, core: 2. Of those that a mesh axis runs over, the one named last changes fastest.
Arguments:
- q_nope: bfloat16 [256, 2048], P('dp'), may hold values from -6 to 6
- q_rope: bfloat16 [256, 1024], P('dp'), may hold values from -40 to 40
- latent_cache: bfloat16 [256, 4096, 512], P('dp', None, 'rank'), may hold values from -6 to 6
- rope_keys: bfloat16 [256, 64, 4096], P('dp', 'rank'), may hold values from -40 to 40
- lengths: int32 [256], P('dp'), may hold values from 1 to 4096, as said below
- slot_of: int32 [256], replicated, may hold values from 0 to 255, as said below
- w_uk: bfloat16 [16, 128, 512], P(None, None, 'rank'), may hold values from -0.5 to 0.5
- w_uv: bfloat16 [16, 512, 128], P(None, 'rank'), may hold values from -1 to 1
- w_out: bfloat16 [2048, 2048], P(None, 'rank'), may hold values from -0.125 to 0.125
Outputs:
- attended: bfloat16 [256, 2048], P('dp', 'rank')
The draws below stay inside these ranges and needn't reach their ends.
Inputs may be any that keep to these rules, and one draw needn't show every extreme that they name: Cache slot j holds lengths[j] live positions, 0 to lengths[j] - 1; some slot holds 4096. `slot_of`: each cache slot belongs to exactly one batch row.
All inputs are finite; a program needn't handle non-finite values.
Results may differ from the reference program's by a relative error of at most 0.014.
Values may be sent and summed in bfloat16 or wider, within the bound.
No kernel may reach another device: no remote copies, remote signals or barrier semaphores. Data moves between devices by JAX's collectives and lax.ppermute only.
A program may use at most 64 MiB of HBM per device.

```python
import math
import jax
import jax.numpy as jnp
from jax import lax

D = 2048
H = 16
NOPE = 128
ROPE = 64
LATENT = 512
VHEAD = 128
SEQ_DEV = 4
CAP = 4096
SEQS = 256


def force_pair(slot_of, row, target):
    inverse = jnp.argsort(slot_of, stable=True).astype(jnp.int32)
    other = inverse[target]
    current = slot_of[row]
    return slot_of.at[other].set(current).at[row].set(target).astype(jnp.int32)


def joint_draw(key):
    key_order = jax.random.fold_in(key, 7001)
    key_upper = jax.random.fold_in(key, 7002)
    key_lower = jax.random.fold_in(key, 7003)
    key_chosen = jax.random.fold_in(key, 7004)
    key_query = jax.random.fold_in(key, 7005)
    key_rope = jax.random.fold_in(key, 7006)
    key_latent = jax.random.fold_in(key, 7007)
    key_pair = jax.random.fold_in(key, 7012)
    key_offset = jax.random.fold_in(key, 7013)
    dev_count = SEQS // SEQ_DEV
    slot_of = jax.random.permutation(key_order, SEQS).astype(jnp.int32)
    first_row = jax.random.randint(key_pair, (), 0, SEQS).astype(jnp.int32)
    first_dev = first_row // SEQ_DEV
    second_row = (first_dev * SEQ_DEV + (first_row % SEQ_DEV + 1) % SEQ_DEV).astype(jnp.int32)
    offsets = jax.random.randint(key_offset, (2,), 0, SEQ_DEV).astype(jnp.int32)
    first_target = ((first_dev + 1) % dev_count * SEQ_DEV + offsets[0]).astype(jnp.int32)
    second_target = ((first_dev + dev_count - 1) % dev_count * SEQ_DEV + offsets[1]).astype(jnp.int32)
    slot_of = force_pair(slot_of, first_row, first_target)
    slot_of = force_pair(slot_of, second_row, second_target)
    upper_bound = jax.random.randint(key_upper, (SEQS,), 1, CAP + 1)
    lengths = jax.random.randint(key_lower, (SEQS,), 1, upper_bound + 1)
    chosen = jax.random.permutation(key_chosen, SEQS)[:3].astype(jnp.int32)
    lengths = lengths.at[chosen].set(CAP)
    lengths = lengths.at[first_target].set(CAP).at[second_target].set(CAP).astype(jnp.int32)
    query_rope = jnp.clip(jax.random.normal(key_query, (SEQS, H * ROPE), jnp.float32), -6.0, 6.0)
    rope_keys = jnp.clip(jax.random.normal(key_rope, (SEQS, ROPE, CAP), jnp.float32), -6.0, 6.0)
    latent = jnp.clip(jax.random.normal(key_latent, (SEQS, CAP, LATENT), jnp.float32), -6.0, 6.0)
    return (slot_of, lengths, query_rope, rope_keys, latent)


def draw_slot_of(key, part):
    return joint_draw(key)[0]


def draw_lengths(key, part):
    return joint_draw(key)[1]


def draw_q_rope(key, part):
    return joint_draw(key)[2].astype(jnp.bfloat16)


def draw_rope_keys(key, part):
    return joint_draw(key)[3].astype(jnp.bfloat16)


def draw_latent_cache(key, part):
    return joint_draw(key)[4].astype(jnp.bfloat16)


def shard_levels(stream_key, shape, pieces, least, top_value):
    loudness = 1.0
    for axis_at, parts in pieces:
        heights = jax.random.uniform(jax.random.fold_in(jax.random.fold_in(stream_key, 6), axis_at), (parts,), jnp.float32, least / len(pieces), top_value / len(pieces))
        loudness = loudness * jnp.repeat(jnp.exp(heights), shape[axis_at] // parts).reshape((-1,) + (1,) * (len(shape) - 1 - axis_at))
    return loudness


def scatter_about(rng, dims, deviation, reach, cuts=(), kind=jnp.bfloat16):
    entries = deviation * jax.random.normal(rng, dims, jnp.float32)
    if cuts:
        entries = entries * shard_levels(rng, dims, cuts, -0.22, 0.18)
    return jnp.clip(entries, -reach, reach).astype(kind)


def setup_inputs(seed: int = 0) -> dict:
    splits = jax.random.split(jax.random.key(seed), 10)
    q_nope = scatter_about(splits[0], (SEQS, H * NOPE), 1.0, 6.0, ((0, 64),))
    q_rope = draw_q_rope(jax.random.fold_in(splits[9], 71), 0)
    latent_cache = draw_latent_cache(jax.random.fold_in(splits[9], 71), 0)
    rope_keys = draw_rope_keys(jax.random.fold_in(splits[9], 71), 0)
    lengths = draw_lengths(jax.random.fold_in(splits[9], 71), 0)
    slot_of = draw_slot_of(jax.random.fold_in(splits[9], 71), 0)
    w_uk = scatter_about(splits[6], (H, NOPE, LATENT), NOPE ** -0.5, 0.5, ((2, 4),))
    w_uv = scatter_about(splits[7], (H, LATENT, VHEAD), (LATENT // 16) ** -0.5, 1.0, ((1, 4),))
    w_out = scatter_about(splits[8], (H * VHEAD, D), (H * VHEAD) ** -0.5, 0.125, ((1, 4),))
    return {"q_nope": q_nope, "q_rope": q_rope, "latent_cache": latent_cache, "rope_keys": rope_keys, "lengths": lengths, "slot_of": slot_of, "w_uk": w_uk, "w_uv": w_uv, "w_out": w_out}


def reference(q_nope, q_rope, latent_cache, rope_keys, lengths, slot_of, w_uk, w_uv, w_out):
    batch_rows = jnp.zeros((SEQS,), jnp.int32).at[slot_of].set(jnp.arange(SEQS, dtype=jnp.int32))
    nope_rows = q_nope[batch_rows].reshape(SEQS, H, NOPE).astype(jnp.float32)
    query_lat = jnp.einsum('shn,hnl->shl', nope_rows, w_uk.astype(jnp.float32)).astype(jnp.bfloat16)
    query_rope = q_rope[batch_rows].reshape(SEQS, H, ROPE)
    score_scale = 1.0 / math.sqrt(NOPE + ROPE)
    positions = jnp.arange(CAP, dtype=jnp.int32)
    up_values = w_uv.astype(jnp.float32)

    def attend(item):
        lat_query, rope_query, cache_rows, key_rows, live_length = item
        scores = jnp.dot(lat_query, cache_rows.T, preferred_element_type=jnp.float32)
        scores = (scores + jnp.dot(rope_query, key_rows, preferred_element_type=jnp.float32)) * score_scale
        scores = jnp.where(positions[None, :] < live_length, scores, -jnp.inf)
        row_max = lax.optimization_barrier(jnp.max(scores, axis=1, keepdims=True))
        raised = jnp.exp(scores - row_max)
        weights = (raised / lax.optimization_barrier(jnp.sum(raised, axis=1, keepdims=True))).astype(jnp.bfloat16)
        latent_out = jnp.dot(weights, cache_rows, preferred_element_type=jnp.float32).astype(jnp.bfloat16)
        head_values = jnp.einsum('hl,hlv->hv', latent_out.astype(jnp.float32), up_values).astype(jnp.bfloat16)
        return jnp.dot(head_values.reshape(H * VHEAD), w_out, preferred_element_type=jnp.float32).astype(jnp.bfloat16)
    slot_out = lax.map(attend, (query_lat, query_rope, latent_cache, rope_keys, lengths))
    return slot_out[slot_of]
```

```python
import math

import jax
import jax.numpy as jnp
from jax import lax
from jax.sharding import PartitionSpec as P

NZ, NX, NC = 8, 4, 2


def dp_groups():
    z_groups = [[z * NX * NC + p for z in range(NZ)] for p in range(NX * NC)]
    x_groups = [[(z * NX + x) * NC + c for x in range(NX)] for z in range(NZ) for c in range(NC)]
    c_groups = [[i * NC + c for c in range(NC)] for i in range(NZ * NX)]
    return z_groups, x_groups, c_groups


def shifted(array, axis, groups, step):
    pairs = [(g[i], g[(i + step) % len(g)]) for g in groups for i in range(len(g))]
    return lax.ppermute(array, axis, pairs)


def from_ranks(arrays):
    count = lax.axis_size("rank")
    return [
        shifted(a, "rank", [list(range(count))], k) for k, a in enumerate(arrays, start=1)
    ]


def per_device(q_nope, q_rope, latent_cache, rope_keys, lengths, slot_of, w_uk, w_uv, w_out):
    f32, bf16 = jnp.float32, jnp.bfloat16
    seqs = q_nope.shape[0]
    heads, nope_dim, lat_part = w_uk.shape
    rope_part = rope_keys.shape[1]
    rope_dim = q_rope.shape[1] // heads
    capacity = latent_cache.shape[1]
    value_dim = w_uv.shape[2]
    seq_total = slot_of.shape[0]
    ranks = lax.axis_size("rank")
    group = heads // ranks
    scale = 1.0 / math.sqrt(nope_dim + rope_dim)
    z_groups, x_groups, c_groups = dp_groups()
    rank_pos = lax.axis_index("rank")
    dp_pos = lax.axis_index("dp")
    c_pos = dp_pos % NC
    x_pos = dp_pos // NC % NX
    z_pos = dp_pos // (NC * NX)

    own_lat = jnp.einsum(
        "shn,hnl->shl", q_nope.reshape(seqs, heads, nope_dim), w_uk, preferred_element_type=f32
    ).astype(bf16).reshape(seqs, heads * lat_part)
    own_rope = lax.dynamic_slice_in_dim(
        q_rope.reshape(seqs, heads, rope_dim), rank_pos * rope_part, rope_part, 2
    ).reshape(seqs, heads * rope_part)
    rows = jnp.concatenate([own_lat, own_rope], axis=1)

    over_x = [rows] + [shifted(rows, "dp", x_groups, k) for k in range(1, NX)]
    over_x = jnp.concatenate(over_x, axis=0)
    plane = jnp.concatenate([over_x, shifted(over_x, "dp", c_groups, 1)], axis=0)
    at = jnp.arange(plane.shape[0], dtype=jnp.int32)
    from_c = (c_pos + at // (NX * seqs)) % NC
    from_x = (x_pos - at // seqs % NX) % NX
    row_of = ((z_pos * NX + from_x) * NC + from_c) * seqs + at % seqs
    slot_here = jnp.sum(
        jnp.where(
            row_of[:, None] == jnp.arange(seq_total, dtype=jnp.int32)[None, :], slot_of[None, :], 0
        ),
        axis=1,
    )
    wanted = jnp.arange(NZ * seqs, dtype=jnp.int32)
    wanted = ((wanted // seqs * NX + x_pos) * NC + c_pos) * seqs + wanted % seqs
    pick = (wanted[:, None] == slot_here[None, :]).astype(bf16)
    picked = jnp.dot(pick, plane, preferred_element_type=f32).astype(bf16)
    arrived = lax.all_to_all(
        picked.reshape(NZ, seqs, -1), "dp", 0, 0, axis_index_groups=z_groups, tiled=True
    )
    query = arrived.astype(f32).sum(axis=0).astype(bf16)
    query_lat = query[:, : heads * lat_part].reshape(seqs, ranks, group, lat_part)
    query_rope = query[:, heads * lat_part :].reshape(seqs, ranks, group, rope_part)

    turned_lat = jnp.roll(query_lat, -rank_pos, axis=1).reshape(seqs, heads, lat_part)
    turned_rope = jnp.roll(query_rope, -rank_pos, axis=1).reshape(seqs, heads, rope_part)
    scores = (
        jnp.einsum("shl,stl->sht", turned_lat, latent_cache, preferred_element_type=f32)
        + jnp.einsum("she,set->sht", turned_rope, rope_keys, preferred_element_type=f32)
    ) * scale
    scores = scores.reshape(seqs, ranks, group, capacity)
    own = scores[:, 0]
    for part in from_ranks([scores[:, k] for k in range(1, ranks)]):
        own = own + part
    positions = jnp.arange(capacity, dtype=jnp.int32)
    own = jnp.where(positions[None, None, :] < lengths[:, None, None], own, -jnp.inf)
    raised = jnp.exp(own - jnp.max(own, axis=2, keepdims=True))
    weights = (raised / jnp.sum(raised, axis=2, keepdims=True)).astype(bf16)

    gathered = [weights] + from_ranks([weights] * (ranks - 1))
    gathered = jnp.concatenate(gathered[::-1], axis=1)
    latent_out = jnp.einsum(
        "sht,stl->shl", gathered, latent_cache, preferred_element_type=f32
    ).astype(bf16)
    latent_out = jnp.roll(
        latent_out.reshape(seqs, ranks, group, lat_part), rank_pos + 1, axis=1
    ).reshape(seqs, heads, lat_part)
    value_part = jnp.einsum(
        "shl,hlv->shv", latent_out, w_uv, preferred_element_type=f32
    ).astype(bf16).reshape(seqs, heads * value_dim)
    total = value_part.astype(f32)
    for part in from_ranks([value_part] * (ranks - 1)):
        total = total + part.astype(f32)
    out_rows = jnp.dot(total.astype(bf16), w_out, preferred_element_type=f32).astype(bf16)

    copies = jnp.broadcast_to(out_rows, (lax.axis_size("dp"), *out_rows.shape))
    everyone = lax.all_to_all(copies, "dp", 0, 0, tiled=True).reshape(seq_total, -1)
    targets = lax.dynamic_slice_in_dim(slot_of, dp_pos * seqs, seqs)
    back = (targets[:, None] == jnp.arange(seq_total, dtype=jnp.int32)[None, :]).astype(bf16)
    return jnp.dot(back, everyone, preferred_element_type=f32).astype(bf16)


def solution(mesh):
    placed = (
        P("dp", None),
        P("dp", None),
        P("dp", None, "rank"),
        P("dp", "rank", None),
        P("dp"),
        P(),
        P(None, None, "rank"),
        P(None, "rank", None),
        P(None, "rank"),
    )
    return jax.shard_map(
        per_device, mesh=mesh, in_specs=placed, out_specs=P("dp", "rank"), check_vma=False
    )
```

```python
import math

import jax
import jax.numpy as jnp
from jax import lax
from jax.experimental import pallas as pl
from jax.experimental.pallas import tpu as pltpu
from jax.sharding import PartitionSpec as P

NZ, NX, NC = 8, 4, 2


def dp_groups():
    z_groups = [[z * NX * NC + p for z in range(NZ)] for p in range(NX * NC)]
    x_groups = [[(z * NX + x) * NC + c for x in range(NX)] for z in range(NZ) for c in range(NC)]
    c_groups = [[i * NC + c for c in range(NC)] for i in range(NZ * NX)]
    return z_groups, x_groups, c_groups


def shifted(array, axis, groups, step):
    pairs = [(g[i], g[(i + step) % len(g)]) for g in groups for i in range(len(g))]
    return lax.ppermute(array, axis, pairs)


def from_ranks(arrays):
    count = lax.axis_size("rank")
    return [
        shifted(a, "rank", [list(range(count))], k) for k, a in enumerate(arrays, start=1)
    ]


F32, BF16 = jnp.float32, jnp.bfloat16
BLOCK = 1024
SMALL = pltpu.CompilerParams(vmem_limit_bytes=16 << 20)


def vmem():
    return pl.BlockSpec(memory_space=pltpu.VMEM)


def dot(a, b):
    return jnp.dot(a, b, preferred_element_type=F32)


def iota(shape, dim):
    return lax.broadcasted_iota(jnp.int32, shape, dim)


def fetch(after, *arrays):
    def body(*refs):
        refs[-1][...] = jnp.zeros(refs[-1].shape, F32)

    return pl.pallas_call(
        body,
        out_shape=jax.ShapeDtypeStruct((8, 128), F32),
        in_specs=[vmem()] * (1 + len(arrays)),
        out_specs=vmem(),
        compiler_params=SMALL,
    )(after, *arrays)


def pick_rows(near, far, slot_here, seqs, token):
    rows, width = near.shape

    def body(near_ref, far_ref, slot_ref, token_ref, out_ref):
        dp = lax.axis_index("dp")
        i = iota((NZ * seqs, 2 * rows), 0)
        wanted = (i // seqs * (NX * NC) + dp % (NX * NC)) * seqs + i % seqs
        pick = jnp.where(slot_ref[...] == wanted, 1.0, 0.0).astype(BF16)
        got = dot(pick[:, :rows], near_ref[...]) + dot(pick[:, rows:], far_ref[...])
        got = got.astype(BF16)
        for z in range(NZ):
            out_ref[z] = got[z * seqs : (z + 1) * seqs]

    return pl.pallas_call(
        body,
        out_shape=jax.ShapeDtypeStruct((NZ, seqs, width), BF16),
        in_specs=[vmem()] * 4,
        out_specs=vmem(),
        compiler_params=SMALL,
    )(near, far, slot_here, token)


def partial_scores(arrived, w_uk, latent_cache, rope_keys, scale):
    seqs, capacity, lat_part = latent_cache.shape
    heads, nope_dim, _ = w_uk.shape
    rope_part = rope_keys.shape[1]
    nope_width = heads * nope_dim
    rope_dim = arrived.shape[2] // heads - nope_dim
    ranks = lax.axis_size("rank")
    group = heads // ranks
    steps = capacity // BLOCK

    def body(arrived_ref, w_ref, cache, keys, *rest):
        outs, (lat_rows,) = rest[:ranks], rest[ranks:]
        rank = lax.axis_index("rank")
        query = arrived_ref[0].astype(F32)
        for z in range(1, NZ):
            query = query + arrived_ref[z].astype(F32)
        for h in range(heads):
            turned = (h // group - rank + ranks) % ranks * group + h % group
            lat_rows[pl.ds(pl.multiple_of(turned * seqs, seqs), seqs), :] = dot(
                query[:, h * nope_dim : (h + 1) * nope_dim].astype(BF16), w_ref[h]
            )
        rope_width = heads * rope_dim
        i, j = iota((rope_width, 128), 0), iota((rope_width, 128), 1)
        fold = (i % rope_dim - rank * rope_part == j) & (j < rope_part)
        fold = jnp.where(fold, 1.0, 0.0).astype(BF16)
        t = iota((heads, rope_width), 0)
        own_head = (t // group + rank) % ranks * group + t % group
        mine = own_head == iota((heads, rope_width), 1) // rope_dim
        for s in range(seqs):
            lat = lat_rows[pl.ds(s, heads, stride=seqs), :].astype(BF16)
            flat = jnp.broadcast_to(query[s : s + 1, nope_width:], (heads, rope_width))
            spread = jnp.where(mine, flat, 0.0).astype(BF16)
            rope = dot(spread, fold).astype(BF16)[:, :rope_part]
            for b in range(steps):
                at = pl.ds(b * BLOCK, BLOCK)
                part = lax.dot_general(
                    lat, cache[s, at, :], (((1,), (1,)), ((), ())), preferred_element_type=F32
                )
                part = (part + dot(rope, keys[s, :, at])) * scale
                for k in range(ranks):
                    outs[k][s * group : (s + 1) * group, at] = part[k * group : (k + 1) * group]

    return pl.pallas_call(
        body,
        out_shape=[jax.ShapeDtypeStruct((seqs * group, capacity), F32)] * ranks,
        in_specs=[vmem()] * 4,
        out_specs=[vmem()] * ranks,
        compiler_params=SMALL,
        scratch_shapes=[pltpu.VMEM((heads * seqs, lat_part), F32)],
    )(arrived, w_uk, latent_cache, rope_keys)


def softmax(parts, live):
    rows, capacity = parts[0].shape

    def body(*refs):
        *part_refs, live_ref, out_ref = refs
        total = part_refs[0][...]
        for ref in part_refs[1:]:
            total = total + ref[...]
        total = jnp.where(iota((rows, capacity), 1) < live_ref[...], total, -jnp.inf)
        raised = jnp.exp(total - jnp.max(total, axis=1, keepdims=True))
        out_ref[...] = (raised / jnp.sum(raised, axis=1, keepdims=True)).astype(BF16)

    return pl.pallas_call(
        body,
        out_shape=jax.ShapeDtypeStruct((rows, capacity), BF16),
        in_specs=[vmem()] * (len(parts) + 1),
        out_specs=vmem(),
        compiler_params=SMALL,
    )(*parts, live)


def head_part(weights, latent_cache, w_uv):
    seqs, capacity, lat_part = latent_cache.shape
    heads, _, value_dim = w_uv.shape
    ranks = len(weights)
    group = heads // ranks
    rows = seqs * group
    steps = capacity // BLOCK

    def body(*refs):
        weight_refs = refs[:ranks]
        cache, w_ref, out_ref, lat_rows = refs[ranks:]
        rank = lax.axis_index("rank")
        for s in range(seqs):
            total = jnp.zeros((ranks * rows, lat_part), F32)
            for b in range(steps):
                at = pl.ds(b * BLOCK, BLOCK)
                block = jnp.concatenate([ref[:, at] for ref in weight_refs], axis=0)
                total = total + dot(block, cache[s, at, :])
            lat_rows[s * ranks * rows : (s + 1) * ranks * rows, :] = total
        for k in range(ranks):
            for i in range(group):
                at = pl.ds(k * rows + i, seqs, stride=ranks * rows + group)
                lat = lat_rows[at, :].astype(BF16)
                head = (rank - k + ranks) % ranks * group + i
                out_ref[:, pl.ds(pl.multiple_of(head * value_dim, value_dim), value_dim)] = dot(
                    lat, w_ref[head]
                ).astype(BF16)

    return pl.pallas_call(
        body,
        out_shape=jax.ShapeDtypeStruct((seqs, heads * value_dim), BF16),
        in_specs=[vmem()] * (ranks + 2),
        out_specs=vmem(),
        compiler_params=SMALL,
        scratch_shapes=[pltpu.VMEM((seqs * ranks * rows, lat_part), F32)],
    )(*weights, latent_cache, w_uv)


def project(parts, w_out, copies):
    seqs = parts[0].shape[0]
    width = w_out.shape[1]

    def body(*refs):
        *part_refs, w_ref, out_ref = refs
        total = part_refs[0][...].astype(F32)
        for ref in part_refs[1:]:
            total = total + ref[...].astype(F32)
        out = dot(total.astype(BF16), w_ref[...]).astype(BF16)
        for d in range(copies):
            out_ref[d] = out

    return pl.pallas_call(
        body,
        out_shape=jax.ShapeDtypeStruct((copies, seqs, width), BF16),
        in_specs=[vmem()] * (len(parts) + 1),
        out_specs=vmem(),
        compiler_params=SMALL,
    )(*parts, w_out)


def bring_back(everyone, targets):
    devices, seqs, width = everyone.shape

    def body(all_ref, target_ref, out_ref):
        row = iota((seqs, width), 0)
        wanted = [jnp.broadcast_to(target_ref[j : j + 1, :], (seqs, width)) for j in range(seqs)]
        lines = [jnp.zeros((seqs, width), F32) for _ in range(seqs)]
        for d in range(devices):
            block = all_ref[d].astype(F32)
            for j in range(seqs):
                lines[j] = jnp.where(wanted[j] == row + d * seqs, block, lines[j])
        for j in range(seqs):
            mine = wanted[j] % seqs == row
            line = jnp.sum(jnp.where(mine, lines[j], 0.0), axis=0, keepdims=True)
            out_ref[j : j + 1, :] = line.astype(BF16)

    return pl.pallas_call(
        body,
        out_shape=jax.ShapeDtypeStruct((seqs, width), BF16),
        in_specs=[vmem()] * 2,
        out_specs=vmem(),
        compiler_params=SMALL,
    )(everyone, targets)


def per_device(q_nope, q_rope, latent_cache, rope_keys, lengths, slot_of, w_uk, w_uv, w_out):
    seqs = q_nope.shape[0]
    heads, nope_dim, _ = w_uk.shape
    scale = 1.0 / math.sqrt(nope_dim + q_rope.shape[1] // heads)
    seq_total = slot_of.shape[0]
    ranks = lax.axis_size("rank")
    z_groups, x_groups, c_groups = dp_groups()

    dp_pos = lax.axis_index("dp")
    plane_rows = 2 * NX * seqs
    at = jnp.arange(plane_rows, dtype=jnp.int32)
    from_c = (dp_pos % NC + at // (NX * seqs)) % NC
    from_x = (dp_pos // NC % NX + NX - at // seqs % NX) % NX
    row_of = ((dp_pos // (NC * NX) * NX + from_x) * NC + from_c) * seqs + at % seqs
    slot_here = jnp.sum(
        jnp.where(
            row_of[:, None] == jnp.arange(seq_total, dtype=jnp.int32)[None, :], slot_of[None, :], 0
        ),
        axis=1,
    ).reshape(1, plane_rows)

    live = jnp.repeat(lengths, heads // ranks).reshape(-1, 1)
    targets = lax.dynamic_slice_in_dim(slot_of, dp_pos * seqs, seqs).reshape(seqs, 1)

    rows = jnp.concatenate([q_nope, q_rope], axis=1)
    near = [rows] + [shifted(rows, "dp", x_groups, k) for k in range(1, NX)]
    near = jnp.concatenate(near, axis=0)
    far = shifted(near, "dp", c_groups, 1)
    token = fetch(rows, latent_cache, rope_keys, w_uk, live, targets)
    picked = pick_rows(near, far, slot_here, seqs, token)
    arrived = lax.all_to_all(picked, "dp", 0, 0, axis_index_groups=z_groups, tiled=True)

    own, *others = partial_scores(arrived, w_uk, latent_cache, rope_keys, scale)
    weights = softmax([own] + from_ranks(others), live)
    gathered = [weights] + from_ranks([weights] * (ranks - 1))
    value_part = head_part(gathered, latent_cache, w_uv)
    parts = [value_part] + from_ranks([value_part] * (ranks - 1))
    copies = project(parts, w_out, lax.axis_size("dp"))
    everyone = lax.all_to_all(copies, "dp", 0, 0, tiled=True)
    return bring_back(everyone, targets)


def solution(mesh):
    placed = (
        P("dp", None),
        P("dp", None),
        P("dp", None, "rank"),
        P("dp", "rank", None),
        P("dp"),
        P(),
        P(None, None, "rank"),
        P(None, "rank", None),
        P(None, "rank"),
    )
    return jax.shard_map(
        per_device, mesh=mesh, in_specs=placed, out_specs=P("dp", "rank"), check_vma=False
    )
```

```python
import math

import jax
import jax.numpy as jnp
from jax import lax
from jax.experimental import pallas as pl
from jax.experimental.pallas import tpu as pltpu
from jax.sharding import PartitionSpec as P

NZ, NX, NC = 8, 4, 2


def dp_groups():
    z_groups = [[z * NX * NC + p for z in range(NZ)] for p in range(NX * NC)]
    x_groups = [[(z * NX + x) * NC + c for x in range(NX)] for z in range(NZ) for c in range(NC)]
    c_groups = [[i * NC + c for c in range(NC)] for i in range(NZ * NX)]
    return z_groups, x_groups, c_groups


def shifted(array, axis, groups, step):
    pairs = [(g[i], g[(i + step) % len(g)]) for g in groups for i in range(len(g))]
    return lax.ppermute(array, axis, pairs)


def from_ranks(arrays):
    count = lax.axis_size("rank")
    return [
        shifted(a, "rank", [list(range(count))], k) for k, a in enumerate(arrays, start=1)
    ]


F32, BF16 = jnp.float32, jnp.bfloat16
BLOCK = 512
SIZES = (9216, 10240, 12288)
SMALL = pltpu.CompilerParams(vmem_limit_bytes=8 << 20)
SCORES = pltpu.CompilerParams(vmem_limit_bytes=8 << 20)
LARGE = pltpu.CompilerParams(vmem_limit_bytes=40 << 20)


def vmem():
    return pl.BlockSpec(memory_space=pltpu.VMEM)


def smem():
    return pl.BlockSpec(memory_space=pltpu.SMEM)


def hbm():
    return pl.BlockSpec(memory_space=pltpu.HBM)


def dot(a, b):
    return jnp.dot(a, b, preferred_element_type=F32)


def iota(shape, dim):
    return lax.broadcasted_iota(jnp.int32, shape, dim)


def join(q_nope, q_rope):
    seqs, nope_width = q_nope.shape
    width = nope_width + q_rope.shape[1]

    def body(nope_ref, rope_ref, out_ref, sems):
        copies = [
            pltpu.make_async_copy(nope_ref, out_ref.at[:, :nope_width], sems.at[0]),
            pltpu.make_async_copy(rope_ref, out_ref.at[:, nope_width:], sems.at[1]),
        ]
        for copy in copies:
            copy.start()
        for copy in copies:
            copy.wait()

    return pl.pallas_call(
        body,
        out_shape=jax.ShapeDtypeStruct((seqs, width), BF16),
        in_specs=[hbm()] * 2,
        out_specs=vmem(),
        scratch_shapes=[pltpu.SemaphoreType.DMA((2,))],
        compiler_params=LARGE,
    )(q_nope, q_rope)


def pick_rows(near, far, slot_here, seqs, ready):
    rows, width = near.shape

    def body(near_ref, far_ref, slot_ref, *rest):
        out_ref = rest[-1]
        dp = lax.axis_index("dp")
        i = iota((NZ * seqs, 2 * rows), 0)
        wanted = (i // seqs * (NX * NC) + dp % (NX * NC)) * seqs + i % seqs
        pick = jnp.where(slot_ref[...] == wanted, 1.0, 0.0).astype(BF16)
        got = dot(pick[:, :rows], near_ref[...]) + dot(pick[:, rows:], far_ref[...])
        got = got.astype(BF16)
        for z in range(NZ):
            out_ref[z] = got[z * seqs : (z + 1) * seqs]

    return pl.pallas_call(
        body,
        out_shape=jax.ShapeDtypeStruct((NZ, seqs, width), BF16),
        in_specs=[vmem()] * (3 + len(ready)),
        out_specs=vmem(),
        compiler_params=SMALL,
    )(near, far, slot_here, *ready)


def live_rows(bounds_ref, pos, slot):
    return (pos >= bounds_ref[slot : slot + 1, :1]) & (pos < bounds_ref[8 + slot : 9 + slot, :1])


def partial_scores(arrived, lengths, w_uk, latent_cache, rope_keys, packed, scale):
    seqs, capacity, lat_part = latent_cache.shape
    heads, nope_dim, _ = w_uk.shape
    rope_part = rope_keys.shape[1]
    nope_width = heads * nope_dim
    rope_dim = arrived.shape[2] // heads - nope_dim
    ranks = lax.axis_size("rank")
    group = heads // ranks
    blocks, half = packed // BLOCK, packed // BLOCK // 2

    def body(arrived_ref, len_ref, w_ref, cache_ref, keys_ref, *rest):
        outs, rest = rest[:ranks], rest[ranks:]
        bounds_ref, cache, keys, lat_rows, lat_slots, rope_slots, sems, key_sems = rest
        rank = lax.axis_index("rank")
        counts = [(len_ref[s] + BLOCK - 1) // BLOCK for s in range(seqs)]
        starts = [jnp.int32(0)]
        for s in range(seqs):
            starts.append(starts[-1] + counts[s])
        slots, copies = [], []
        for b in range(blocks):
            slot = jnp.int32(0)
            start = jnp.int32(0)
            for s in range(1, seqs):
                slot = jnp.where(b >= starts[s], s, slot)
                start = jnp.where(b >= starts[s], starts[s], start)
            block = jnp.minimum(b - start, capacity // BLOCK - 1)
            source = pl.ds(pl.multiple_of(block * BLOCK, BLOCK), BLOCK)
            at = pl.ds(b * BLOCK, BLOCK)
            copies.append(
                (
                    pltpu.make_async_copy(cache_ref.at[slot, source], cache.at[at], sems.at[b]),
                    pltpu.make_async_copy(
                        keys_ref.at[slot, :, source], keys.at[:, at], key_sems.at[b]
                    ),
                )
            )
            for copy in copies[-1]:
                copy.start()
            slots.append(slot)
        for s in range(seqs):
            first = starts[s] * BLOCK
            bounds_ref[s : s + 1, :] = jnp.full((1, 128), first, jnp.int32)
            bounds_ref[8 + s : 9 + s, :] = jnp.full((1, 128), first + len_ref[s], jnp.int32)
        query = arrived_ref[0].astype(F32)
        for z in range(1, NZ):
            query = query + arrived_ref[z].astype(F32)
        for h in range(heads):
            turned = (h // group - rank + ranks) % ranks * group + h % group
            lat_rows[pl.ds(pl.multiple_of(turned * seqs, seqs), seqs), :] = dot(
                query[:, h * nope_dim : (h + 1) * nope_dim].astype(BF16), w_ref[h]
            )
        rope_width = heads * rope_dim
        i, j = iota((rope_width, 128), 0), iota((rope_width, 128), 1)
        fold = (i % rope_dim - rank * rope_part == j) & (j < rope_part)
        fold = jnp.where(fold, 1.0, 0.0).astype(BF16)
        t = iota((heads, rope_width), 0)
        own_head = (t // group + rank) % ranks * group + t % group
        mine = own_head == iota((heads, rope_width), 1) // rope_dim
        for s in range(seqs):
            lat_slots[s] = lat_rows[pl.ds(s, heads, stride=seqs), :].astype(BF16)
            flat = jnp.broadcast_to(query[s : s + 1, nope_width:], (heads, rope_width))
            rope_slots[s] = dot(jnp.where(mine, flat, 0.0).astype(BF16), fold).astype(BF16)
        for b in range(blocks):
            for copy in copies[b]:
                copy.wait()
            at = pl.ds(b * BLOCK, BLOCK)
            part = lax.dot_general(
                lat_slots[slots[b]],
                cache[at, :],
                (((1,), (1,)), ((), ())),
                preferred_element_type=F32,
            )
            part = (part + dot(rope_slots[slots[b]][:, :rope_part], keys[:, at])) * scale
            row, to = b // half * group, pl.ds(b % half * BLOCK, BLOCK)
            for k in range(ranks):
                outs[k][row : row + group, to] = part[k * group : (k + 1) * group]

    return pl.pallas_call(
        body,
        out_shape=[jax.ShapeDtypeStruct((2 * group, packed // 2), F32)] * ranks
        + [
            jax.ShapeDtypeStruct((16, 128), jnp.int32),
            jax.ShapeDtypeStruct((packed, lat_part), BF16),
        ],
        in_specs=[vmem(), smem(), vmem(), hbm(), hbm()],
        out_specs=[vmem()] * (ranks + 2),
        compiler_params=SCORES,
        scratch_shapes=[
            pltpu.VMEM((rope_part, packed), BF16),
            pltpu.VMEM((heads * seqs, lat_part), F32),
            pltpu.VMEM((seqs, heads, lat_part), BF16),
            pltpu.VMEM((seqs, heads, 128), BF16),
            pltpu.SemaphoreType.DMA((blocks,)),
            pltpu.SemaphoreType.DMA((blocks,)),
        ],
    )(arrived, lengths, w_uk, latent_cache, rope_keys)


def softmax(parts, bounds, seqs):
    rows, width = parts[0].shape

    def body(*refs):
        *part_refs, bounds_ref, out_ref = refs
        total = part_refs[0][...]
        for ref in part_refs[1:]:
            total = total + ref[...]
        pos = iota((rows, width), 1) + iota((rows, width), 0) // (rows // 2) * width
        live = [live_rows(bounds_ref, pos, s) for s in range(seqs)]
        top = jnp.full((rows, width), jnp.inf, F32)
        for s in range(seqs):
            most = jnp.max(jnp.where(live[s], total, -jnp.inf), axis=1, keepdims=True)
            most = jnp.maximum(most, jnp.concatenate([most[rows // 2 :], most[: rows // 2]], axis=0))
            top = jnp.where(live[s], most, top)
        raised = jnp.exp(jnp.where(top < jnp.inf, total - top, -jnp.inf))
        below = jnp.ones((rows, width), F32)
        for s in range(seqs):
            sums = jnp.sum(jnp.where(live[s], raised, 0.0), axis=1, keepdims=True)
            sums = sums + jnp.concatenate([sums[rows // 2 :], sums[: rows // 2]], axis=0)
            below = jnp.where(live[s], sums, below)
        out_ref[...] = (raised / below).astype(BF16)

    return pl.pallas_call(
        body,
        out_shape=jax.ShapeDtypeStruct((rows, width), BF16),
        in_specs=[vmem()] * (len(parts) + 1),
        out_specs=vmem(),
        compiler_params=SMALL,
    )(*parts, bounds)


def head_part(weights, bounds, cache, w_uv, seqs):
    packed, lat_part = cache.shape
    heads, _, value_dim = w_uv.shape
    ranks = len(weights)
    group = heads // ranks
    blocks, half = packed // BLOCK, packed // BLOCK // 2

    def body(*refs):
        weight_refs = refs[:ranks]
        bounds_ref, cache_ref, w_ref, out_ref, lat_rows = refs[ranks:]
        rank = lax.axis_index("rank")
        total = jnp.zeros((seqs * heads, lat_part), F32)
        for b in range(blocks):
            row, source = b // half * group, pl.ds(b % half * BLOCK, BLOCK)
            block = jnp.concatenate(
                [ref[:, source].astype(F32)[row : row + group] for ref in weight_refs], axis=0
            )
            pos = iota((heads, BLOCK), 1) + b * BLOCK
            block = jnp.concatenate(
                [
                    jnp.where(live_rows(bounds_ref, pos, s), block, 0.0).astype(BF16)
                    for s in range(seqs)
                ],
                axis=0,
            )
            total = total + dot(block, cache_ref[pl.ds(b * BLOCK, BLOCK), :])
        lat_rows[...] = total
        for k in range(ranks):
            for i in range(group):
                lat = lat_rows[pl.ds(k * group + i, seqs, stride=heads), :].astype(BF16)
                head = (rank - k + ranks) % ranks * group + i
                out_ref[:, pl.ds(pl.multiple_of(head * value_dim, value_dim), value_dim)] = dot(
                    lat, w_ref[head]
                ).astype(BF16)

    return pl.pallas_call(
        body,
        out_shape=jax.ShapeDtypeStruct((seqs, heads * value_dim), BF16),
        in_specs=[vmem()] * (ranks + 3),
        out_specs=vmem(),
        compiler_params=SMALL,
        scratch_shapes=[pltpu.VMEM((seqs * heads, lat_part), F32)],
    )(*weights, bounds, cache, w_uv)


def project(parts, w_out, copies):
    seqs = parts[0].shape[0]
    width = w_out.shape[1]

    def body(*refs):
        *part_refs, w_ref, out_ref = refs
        total = part_refs[0][...].astype(F32)
        for ref in part_refs[1:]:
            total = total + ref[...].astype(F32)
        out = dot(total.astype(BF16), w_ref[...]).astype(BF16)
        for d in range(copies):
            out_ref[d] = out

    return pl.pallas_call(
        body,
        out_shape=jax.ShapeDtypeStruct((copies, seqs, width), BF16),
        in_specs=[vmem()] * (len(parts) + 1),
        out_specs=vmem(),
        compiler_params=SMALL,
    )(*parts, w_out)


def bring_back(everyone, targets):
    devices, seqs, width = everyone.shape

    def body(all_ref, target_ref, out_ref):
        row = iota((seqs, width), 0)
        wanted = [jnp.broadcast_to(target_ref[j : j + 1, :], (seqs, width)) for j in range(seqs)]
        lines = [jnp.zeros((seqs, width), F32) for _ in range(seqs)]
        for d in range(devices):
            block = all_ref[d].astype(F32)
            for j in range(seqs):
                lines[j] = jnp.where(wanted[j] == row + d * seqs, block, lines[j])
        for j in range(seqs):
            mine = wanted[j] % seqs == row
            line = jnp.sum(jnp.where(mine, lines[j], 0.0), axis=0, keepdims=True)
            out_ref[j : j + 1, :] = line.astype(BF16)

    return pl.pallas_call(
        body,
        out_shape=jax.ShapeDtypeStruct((seqs, width), BF16),
        in_specs=[vmem()] * 2,
        out_specs=vmem(),
        compiler_params=SMALL,
    )(everyone, targets)


def per_device(q_nope, q_rope, latent_cache, rope_keys, lengths, slot_of, w_uk, w_uv, w_out):
    seqs = q_nope.shape[0]
    heads, nope_dim, _ = w_uk.shape
    scale = 1.0 / math.sqrt(nope_dim + q_rope.shape[1] // heads)
    seq_total = slot_of.shape[0]
    ranks = lax.axis_size("rank")
    z_groups, x_groups, c_groups = dp_groups()

    dp_pos = lax.axis_index("dp")
    plane_rows = 2 * NX * seqs
    at = jnp.arange(plane_rows, dtype=jnp.int32)
    from_c = (dp_pos % NC + at // (NX * seqs)) % NC
    from_x = (dp_pos // NC % NX + NX - at // seqs % NX) % NX
    row_of = ((dp_pos // (NC * NX) * NX + from_x) * NC + from_c) * seqs + at % seqs
    slot_here = jnp.sum(
        jnp.where(
            row_of[:, None] == jnp.arange(seq_total, dtype=jnp.int32)[None, :], slot_of[None, :], 0
        ),
        axis=1,
    ).reshape(1, plane_rows)

    targets = lax.dynamic_slice_in_dim(slot_of, dp_pos * seqs, seqs).reshape(seqs, 1)

    sizes = [n for n in SIZES if n < seqs * latent_cache.shape[1]] + [seqs * latent_cache.shape[1]]
    needed = jnp.sum((lengths + BLOCK - 1) // BLOCK) * BLOCK
    which = sum((needed > n).astype(jnp.int32) for n in sizes[:-1])

    rows = join(q_nope, q_rope)
    near = [rows] + [shifted(rows, "dp", x_groups, k) for k in range(1, NX)]
    near = jnp.concatenate(near, axis=0)
    far = shifted(near, "dp", c_groups, 1)
    picked = pick_rows(near, far, slot_here, seqs, (targets, which.reshape(1, 1)))
    arrived = lax.all_to_all(picked, "dp", 0, 0, axis_index_groups=z_groups, tiled=True)

    def attend(packed):
        def branch(arrived, lengths, w_uk, latent_cache, rope_keys, w_uv):
            own, *others, bounds, cache = partial_scores(
                arrived, lengths, w_uk, latent_cache, rope_keys, packed, scale
            )
            weights = softmax([own] + from_ranks(others), bounds, seqs)
            gathered = [weights] + from_ranks([weights] * (ranks - 1))
            return head_part(gathered, bounds, cache, w_uv, seqs)

        return branch

    value_part = lax.switch(
        which,
        [attend(n) for n in sizes],
        arrived,
        lengths,
        w_uk,
        latent_cache,
        rope_keys,
        w_uv,
    )
    parts = [value_part] + from_ranks([value_part] * (ranks - 1))
    copies = project(parts, w_out, lax.axis_size("dp"))
    everyone = lax.all_to_all(copies, "dp", 0, 0, tiled=True)
    return bring_back(everyone, targets)


def solution(mesh):
    placed = (
        P("dp", None),
        P("dp", None),
        P("dp", None, "rank"),
        P("dp", "rank", None),
        P("dp"),
        P(),
        P(None, None, "rank"),
        P(None, "rank", None),
        P(None, "rank"),
    )
    return jax.shard_map(
        per_device, mesh=mesh, in_specs=placed, out_specs=P("dp", "rank"), check_vma=False
    )
```

```python
import math

import jax
import jax.numpy as jnp
from jax import lax
from jax.experimental import pallas as pl
from jax.experimental.pallas import tpu as pltpu
from jax.sharding import PartitionSpec as P

NZ, NX, NC = 8, 4, 2


def dp_groups():
    z_groups = [[z * NX * NC + p for z in range(NZ)] for p in range(NX * NC)]
    x_groups = [[(z * NX + x) * NC + c for x in range(NX)] for z in range(NZ) for c in range(NC)]
    c_groups = [[i * NC + c for c in range(NC)] for i in range(NZ * NX)]
    return z_groups, x_groups, c_groups


def shifted(array, axis, groups, step):
    pairs = [(g[i], g[(i + step) % len(g)]) for g in groups for i in range(len(g))]
    return lax.ppermute(array, axis, pairs)


def from_ranks(arrays):
    count = lax.axis_size("rank")
    return [
        shifted(a, "rank", [list(range(count))], k) for k, a in enumerate(arrays, start=1)
    ]


F32, BF16 = jnp.float32, jnp.bfloat16
BLOCK = 512
CHUNK = 4
SIZES = (9216, 10240, 12288)
SMALL = pltpu.CompilerParams(vmem_limit_bytes=8 << 20)
LARGE = pltpu.CompilerParams(vmem_limit_bytes=60 << 20)
HALF = pltpu.CompilerParams(vmem_limit_bytes=40 << 20)


def vmem():
    return pl.BlockSpec(memory_space=pltpu.VMEM)


def smem():
    return pl.BlockSpec(memory_space=pltpu.SMEM)


def hbm():
    return pl.BlockSpec(memory_space=pltpu.HBM)


def dot(a, b):
    return jnp.dot(a, b, preferred_element_type=F32)


def iota(shape, dim):
    return lax.broadcasted_iota(jnp.int32, shape, dim)


def join(q_nope, q_rope):
    seqs, nope_width = q_nope.shape
    width = nope_width + q_rope.shape[1]

    def body(nope_ref, rope_ref, out_ref, sems):
        copies = [
            pltpu.make_async_copy(nope_ref, out_ref.at[:, :nope_width], sems.at[0]),
            pltpu.make_async_copy(rope_ref, out_ref.at[:, nope_width:], sems.at[1]),
        ]
        for copy in copies:
            copy.start()
        for copy in copies:
            copy.wait()

    return pl.pallas_call(
        body,
        out_shape=jax.ShapeDtypeStruct((seqs, width), BF16),
        in_specs=[hbm()] * 2,
        out_specs=vmem(),
        scratch_shapes=[pltpu.SemaphoreType.DMA((2,))],
        compiler_params=HALF,
    )(q_nope, q_rope)


def pick_rows(near, far, slot_here, seqs):
    rows, width = near.shape

    def body(near_ref, far_ref, slot_ref, out_ref):
        dp = lax.axis_index("dp")
        i = iota((NZ * seqs, 2 * rows), 0)
        wanted = (i // seqs * (NX * NC) + dp % (NX * NC)) * seqs + i % seqs
        pick = jnp.where(slot_ref[...] == wanted, 1.0, 0.0).astype(BF16)
        got = dot(pick[:, :rows], near_ref[...]) + dot(pick[:, rows:], far_ref[...])
        got = got.astype(BF16)
        for z in range(NZ):
            out_ref[z] = got[z * seqs : (z + 1) * seqs]

    return pl.pallas_call(
        body,
        out_shape=jax.ShapeDtypeStruct((NZ, seqs, width), BF16),
        in_specs=[vmem()] * 3,
        out_specs=vmem(),
        compiler_params=SMALL,
    )(near, far, slot_here)


def pack_live(lengths, latent_cache, rope_keys, ready):
    seqs, capacity, lat_part = latent_cache.shape
    rope_part = rope_keys.shape[1]
    packed = seqs * capacity
    blocks = packed // BLOCK

    def body(len_ref, cache_ref, keys_ref, *rest):
        cache, keys, bounds_ref, sems = rest[-4:]
        starts = [jnp.int32(0)]
        for s in range(seqs):
            starts.append(starts[-1] + (len_ref[s] + BLOCK - 1) // BLOCK)
        copies = []
        for b in range(blocks):
            slot = jnp.int32(0)
            start = jnp.int32(0)
            for s in range(1, seqs):
                slot = jnp.where(b >= starts[s], s, slot)
                start = jnp.where(b >= starts[s], starts[s], start)
            block = jnp.minimum(b - start, capacity // BLOCK - 1)
            source = pl.ds(pl.multiple_of(block * BLOCK, BLOCK), BLOCK)
            at = pl.ds(b * BLOCK, BLOCK)
            copies += [
                pltpu.make_async_copy(cache_ref.at[slot, source], cache.at[at], sems.at[0, b]),
                pltpu.make_async_copy(keys_ref.at[slot, :, source], keys.at[:, at], sems.at[1, b]),
            ]
            copies[-2].start()
            copies[-1].start()
        for s in range(seqs):
            first = starts[s] * BLOCK
            bounds_ref[s : s + 1, :] = jnp.full((1, 128), first, jnp.int32)
            bounds_ref[8 + s : 9 + s, :] = jnp.full((1, 128), first + len_ref[s], jnp.int32)
        for copy in copies:
            copy.wait()

    return pl.pallas_call(
        body,
        out_shape=[
            jax.ShapeDtypeStruct((packed, lat_part), BF16),
            jax.ShapeDtypeStruct((rope_part, packed), BF16),
            jax.ShapeDtypeStruct((16, 128), jnp.int32),
        ],
        in_specs=[smem(), hbm(), hbm()] + [hbm()] * len(ready),
        out_specs=[vmem()] * 3,
        compiler_params=LARGE,
        scratch_shapes=[pltpu.SemaphoreType.DMA((2, blocks))],
    )(lengths, latent_cache, rope_keys, *ready)


def absorb(arrived, w_uk, rope_part):
    _, seqs, width = arrived.shape
    heads, nope_dim, lat_part = w_uk.shape
    nope_width = heads * nope_dim
    rope_dim = width // heads - nope_dim
    ranks = lax.axis_size("rank")
    group = heads // ranks

    def body(arrived_ref, w_ref, lat_ref, rope_ref, lat_rows):
        rank = lax.axis_index("rank")
        query = arrived_ref[0].astype(F32)
        for z in range(1, NZ):
            query = query + arrived_ref[z].astype(F32)
        for h in range(heads):
            turned = (h // group - rank + ranks) % ranks * group + h % group
            lat_rows[pl.ds(pl.multiple_of(turned * seqs, seqs), seqs), :] = dot(
                query[:, h * nope_dim : (h + 1) * nope_dim].astype(BF16), w_ref[h]
            )
        rope_width = heads * rope_dim
        i, j = iota((rope_width, 128), 0), iota((rope_width, 128), 1)
        fold = (i % rope_dim - rank * rope_part == j) & (j < rope_part)
        fold = jnp.where(fold, 1.0, 0.0).astype(BF16)
        t = iota((heads, rope_width), 0)
        own_head = (t // group + rank) % ranks * group + t % group
        mine = own_head == iota((heads, rope_width), 1) // rope_dim
        for s in range(seqs):
            rows = slice(s * heads, (s + 1) * heads)
            lat_ref[rows, :] = lat_rows[pl.ds(s, heads, stride=seqs), :].astype(BF16)
            flat = jnp.broadcast_to(query[s : s + 1, nope_width:], (heads, rope_width))
            rope_ref[rows, :] = dot(jnp.where(mine, flat, 0.0).astype(BF16), fold).astype(BF16)

    return pl.pallas_call(
        body,
        out_shape=[
            jax.ShapeDtypeStruct((seqs * heads, lat_part), BF16),
            jax.ShapeDtypeStruct((seqs * heads, 128), BF16),
        ],
        in_specs=[vmem()] * 2,
        out_specs=[vmem()] * 2,
        compiler_params=SMALL,
        scratch_shapes=[pltpu.VMEM((heads * seqs, lat_part), F32)],
    )(arrived, w_uk)


def live_rows(bounds_ref, pos, slot):
    return (pos >= bounds_ref[slot : slot + 1, :1]) & (pos < bounds_ref[8 + slot : 9 + slot, :1])


def partial_scores(query_lat, query_rope, bounds, cache, keys, packed, seqs, scale):
    heads, lat_part = query_lat.shape[0] // seqs, query_lat.shape[1]
    rope_part = keys.shape[0]
    ranks = lax.axis_size("rank")
    group = heads // ranks
    blocks, half = packed // BLOCK, packed // BLOCK // 2
    chunks = [(b, min(b + CHUNK, blocks)) for b in range(0, blocks, CHUNK)]

    def body(lat_ref, rope_ref, bounds_ref, cache_hbm, keys_hbm, *rest):
        outs, (cache_ref, keys_ref, sems) = rest[:ranks], rest[ranks:]
        copies = []
        for i, (first, end) in enumerate(chunks):
            at = pl.ds(first * BLOCK, (end - first) * BLOCK)
            copies += [
                pltpu.make_async_copy(cache_hbm.at[at], cache_ref.at[at], sems.at[0, i]),
                pltpu.make_async_copy(keys_hbm.at[:, at], keys_ref.at[:, at], sems.at[1, i]),
            ]
            copies[-2].start()
            copies[-1].start()
        lat, rope = lat_ref[...], rope_ref[:, :rope_part]
        for b in range(blocks):
            if b % CHUNK == 0:
                copies[b // CHUNK * 2].wait()
                copies[b // CHUNK * 2 + 1].wait()
            at = pl.ds(b * BLOCK, BLOCK)
            every = lax.dot_general(
                lat, cache_ref[at, :], (((1,), (1,)), ((), ())), preferred_element_type=F32
            )
            every = every + dot(rope, keys_ref[:, at])
            pos = iota((heads, BLOCK), 1) + b * BLOCK
            part = every[:heads]
            for s in range(1, seqs):
                rows = every[s * heads : (s + 1) * heads]
                part = jnp.where(pos >= bounds_ref[s : s + 1, :1], rows, part)
            part = part * scale
            row, to = b // half * group, pl.ds(b % half * BLOCK, BLOCK)
            for k in range(ranks):
                outs[k][row : row + group, to] = part[k * group : (k + 1) * group]

    return pl.pallas_call(
        body,
        out_shape=[jax.ShapeDtypeStruct((2 * group, packed // 2), F32)] * ranks
        + [jax.ShapeDtypeStruct((packed, lat_part), BF16)],
        in_specs=[vmem()] * 3 + [hbm()] * 2,
        out_specs=[vmem()] * (ranks + 1),
        compiler_params=SMALL,
        scratch_shapes=[
            pltpu.VMEM((rope_part, packed), BF16),
            pltpu.SemaphoreType.DMA((2, len(chunks))),
        ],
    )(query_lat, query_rope, bounds, cache, keys)


def softmax(parts, bounds, seqs):
    rows, width = parts[0].shape

    def body(*refs):
        *part_refs, bounds_ref, out_ref = refs
        total = part_refs[0][...]
        for ref in part_refs[1:]:
            total = total + ref[...]
        pos = iota((rows, width), 1) + iota((rows, width), 0) // (rows // 2) * width
        live = [live_rows(bounds_ref, pos, s) for s in range(seqs)]
        top = jnp.full((rows, width), jnp.inf, F32)
        for s in range(seqs):
            most = jnp.max(jnp.where(live[s], total, -jnp.inf), axis=1, keepdims=True)
            most = jnp.maximum(most, jnp.concatenate([most[rows // 2 :], most[: rows // 2]], axis=0))
            top = jnp.where(live[s], most, top)
        raised = jnp.exp(jnp.where(top < jnp.inf, total - top, -jnp.inf))
        below = jnp.ones((rows, width), F32)
        for s in range(seqs):
            sums = jnp.sum(jnp.where(live[s], raised, 0.0), axis=1, keepdims=True)
            sums = sums + jnp.concatenate([sums[rows // 2 :], sums[: rows // 2]], axis=0)
            below = jnp.where(live[s], sums, below)
        out_ref[...] = (raised / below).astype(BF16)

    return pl.pallas_call(
        body,
        out_shape=jax.ShapeDtypeStruct((rows, width), BF16),
        in_specs=[vmem()] * (len(parts) + 1),
        out_specs=vmem(),
        compiler_params=SMALL,
    )(*parts, bounds)


def head_part(weights, bounds, cache, w_uv, packed, seqs):
    heads, lat_part, value_dim = w_uv.shape
    ranks = len(weights)
    group = heads // ranks
    blocks, half = packed // BLOCK, packed // BLOCK // 2

    def body(*refs):
        weight_refs = refs[:ranks]
        bounds_ref, cache_ref, w_ref, out_ref, lat_rows = refs[ranks:]
        rank = lax.axis_index("rank")
        total = jnp.zeros((seqs * heads, lat_part), F32)
        for b in range(blocks):
            row, source = b // half * group, pl.ds(b % half * BLOCK, BLOCK)
            block = jnp.concatenate(
                [ref[:, source].astype(F32)[row : row + group] for ref in weight_refs], axis=0
            )
            pos = iota((heads, BLOCK), 1) + b * BLOCK
            block = jnp.concatenate(
                [
                    jnp.where(live_rows(bounds_ref, pos, s), block, 0.0).astype(BF16)
                    for s in range(seqs)
                ],
                axis=0,
            )
            total = total + dot(block, cache_ref[pl.ds(b * BLOCK, BLOCK), :])
        lat_rows[...] = total
        for k in range(ranks):
            for i in range(group):
                lat = lat_rows[pl.ds(k * group + i, seqs, stride=heads), :].astype(BF16)
                head = (rank - k + ranks) % ranks * group + i
                out_ref[:, pl.ds(pl.multiple_of(head * value_dim, value_dim), value_dim)] = dot(
                    lat, w_ref[head]
                ).astype(BF16)

    return pl.pallas_call(
        body,
        out_shape=jax.ShapeDtypeStruct((seqs, heads * value_dim), BF16),
        in_specs=[vmem()] * (ranks + 3),
        out_specs=vmem(),
        compiler_params=SMALL,
        scratch_shapes=[pltpu.VMEM((seqs * heads, lat_part), F32)],
    )(*weights, bounds, cache, w_uv)


def project(parts, w_out, copies):
    seqs = parts[0].shape[0]
    width = w_out.shape[1]

    def body(*refs):
        *part_refs, w_ref, out_ref = refs
        total = part_refs[0][...].astype(F32)
        for ref in part_refs[1:]:
            total = total + ref[...].astype(F32)
        out = dot(total.astype(BF16), w_ref[...]).astype(BF16)
        for d in range(copies):
            out_ref[d] = out

    return pl.pallas_call(
        body,
        out_shape=jax.ShapeDtypeStruct((copies, seqs, width), BF16),
        in_specs=[vmem()] * (len(parts) + 1),
        out_specs=vmem(),
        compiler_params=SMALL,
    )(*parts, w_out)


def bring_back(everyone, targets):
    devices, seqs, width = everyone.shape

    def body(all_ref, target_ref, out_ref):
        row = iota((seqs, width), 0)
        wanted = [jnp.broadcast_to(target_ref[j : j + 1, :], (seqs, width)) for j in range(seqs)]
        lines = [jnp.zeros((seqs, width), F32) for _ in range(seqs)]
        for d in range(devices):
            block = all_ref[d].astype(F32)
            for j in range(seqs):
                lines[j] = jnp.where(wanted[j] == row + d * seqs, block, lines[j])
        for j in range(seqs):
            mine = wanted[j] % seqs == row
            line = jnp.sum(jnp.where(mine, lines[j], 0.0), axis=0, keepdims=True)
            out_ref[j : j + 1, :] = line.astype(BF16)

    return pl.pallas_call(
        body,
        out_shape=jax.ShapeDtypeStruct((seqs, width), BF16),
        in_specs=[vmem()] * 2,
        out_specs=vmem(),
        compiler_params=SMALL,
    )(everyone, targets)


def per_device(q_nope, q_rope, latent_cache, rope_keys, lengths, slot_of, w_uk, w_uv, w_out):
    seqs = q_nope.shape[0]
    heads, nope_dim, _ = w_uk.shape
    scale = 1.0 / math.sqrt(nope_dim + q_rope.shape[1] // heads)
    seq_total = slot_of.shape[0]
    ranks = lax.axis_size("rank")
    z_groups, x_groups, c_groups = dp_groups()

    dp_pos = lax.axis_index("dp")
    plane_rows = 2 * NX * seqs
    at = jnp.arange(plane_rows, dtype=jnp.int32)
    from_c = (dp_pos % NC + at // (NX * seqs)) % NC
    from_x = (dp_pos // NC % NX + NX - at // seqs % NX) % NX
    row_of = ((dp_pos // (NC * NX) * NX + from_x) * NC + from_c) * seqs + at % seqs
    slot_here = jnp.sum(
        jnp.where(
            row_of[:, None] == jnp.arange(seq_total, dtype=jnp.int32)[None, :], slot_of[None, :], 0
        ),
        axis=1,
    ).reshape(1, plane_rows)

    targets = lax.dynamic_slice_in_dim(slot_of, dp_pos * seqs, seqs).reshape(seqs, 1)

    sizes = [n for n in SIZES if n < seqs * latent_cache.shape[1]] + [seqs * latent_cache.shape[1]]
    needed = jnp.sum((lengths + BLOCK - 1) // BLOCK) * BLOCK
    which = sum((needed > n).astype(jnp.int32) for n in sizes[:-1])

    rows = join(q_nope, q_rope)
    near = [rows] + [shifted(rows, "dp", x_groups, k) for k in range(1, NX)]
    near = jnp.concatenate(near, axis=0)
    far = shifted(near, "dp", c_groups, 1)
    picked = pick_rows(near, far, slot_here, seqs)
    cache, keys, bounds = pack_live(
        lengths, latent_cache, rope_keys, (picked, targets, which.reshape(1, 1))
    )
    arrived = lax.all_to_all(picked, "dp", 0, 0, axis_index_groups=z_groups, tiled=True)

    query_lat, query_rope = absorb(arrived, w_uk, rope_keys.shape[1])

    def attend(packed):
        def branch(query_lat, query_rope, bounds, cache, keys, w_uv):
            own, *others, held = partial_scores(
                query_lat, query_rope, bounds, cache, keys, packed, seqs, scale
            )
            weights = softmax([own] + from_ranks(others), bounds, seqs)
            gathered = [weights] + from_ranks([weights] * (ranks - 1))
            return head_part(gathered, bounds, held, w_uv, packed, seqs)

        return branch

    value_part = lax.switch(
        which, [attend(n) for n in sizes], query_lat, query_rope, bounds, cache, keys, w_uv
    )
    parts = [value_part] + from_ranks([value_part] * (ranks - 1))
    copies = project(parts, w_out, lax.axis_size("dp"))
    everyone = lax.all_to_all(copies, "dp", 0, 0, tiled=True)
    return bring_back(everyone, targets)


def solution(mesh):
    placed = (
        P("dp", None),
        P("dp", None),
        P("dp", None, "rank"),
        P("dp", "rank", None),
        P("dp"),
        P(),
        P(None, None, "rank"),
        P(None, "rank", None),
        P(None, "rank"),
    )
    return jax.shard_map(
        per_device, mesh=mesh, in_specs=placed, out_specs=P("dp", "rank"), check_vma=False
    )
```

```python
import math

import jax
import jax.numpy as jnp
from jax import lax
from jax.experimental import pallas as pl
from jax.experimental.pallas import tpu as pltpu
from jax.sharding import PartitionSpec as P

NZ, NX, NC = 8, 4, 2


def dp_groups():
    z_groups = [[z * NX * NC + p for z in range(NZ)] for p in range(NX * NC)]
    x_groups = [[(z * NX + x) * NC + c for x in range(NX)] for z in range(NZ) for c in range(NC)]
    c_groups = [[i * NC + c for c in range(NC)] for i in range(NZ * NX)]
    return z_groups, x_groups, c_groups


def shifted(array, axis, groups, step):
    pairs = [(g[i], g[(i + step) % len(g)]) for g in groups for i in range(len(g))]
    return lax.ppermute(array, axis, pairs)


def from_ranks(arrays):
    count = lax.axis_size("rank")
    return [
        shifted(a, "rank", [list(range(count))], k) for k, a in enumerate(arrays, start=1)
    ]


F32, BF16 = jnp.float32, jnp.bfloat16
BLOCK = 512
SIZES = (9216, 10240, 12288)
SMALL = pltpu.CompilerParams(vmem_limit_bytes=8 << 20)


def vmem():
    return pl.BlockSpec(memory_space=pltpu.VMEM)


def smem():
    return pl.BlockSpec(memory_space=pltpu.SMEM)


def hbm():
    return pl.BlockSpec(memory_space=pltpu.HBM)


def dot(a, b):
    return jnp.dot(a, b, preferred_element_type=F32)


def iota(shape, dim):
    return lax.broadcasted_iota(jnp.int32, shape, dim)


def join(q_nope, q_rope):
    seqs, nope_width = q_nope.shape
    width = nope_width + q_rope.shape[1]

    def body(nope_ref, rope_ref, out_ref, sems):
        copies = [
            pltpu.make_async_copy(nope_ref, out_ref.at[:, :nope_width], sems.at[0]),
            pltpu.make_async_copy(rope_ref, out_ref.at[:, nope_width:], sems.at[1]),
        ]
        for copy in copies:
            copy.start()
        for copy in copies:
            copy.wait()

    return pl.pallas_call(
        body,
        out_shape=jax.ShapeDtypeStruct((seqs, width), BF16),
        in_specs=[hbm()] * 2,
        out_specs=vmem(),
        scratch_shapes=[pltpu.SemaphoreType.DMA((2,))],
        compiler_params=SMALL,
    )(q_nope, q_rope)


def pick_rows(near, far, slot_here, seqs, ready):
    rows, width = near.shape

    def body(near_ref, far_ref, slot_ref, *rest):
        out_ref = rest[-1]
        dp = lax.axis_index("dp")
        i = iota((NZ * seqs, 2 * rows), 0)
        wanted = (i // seqs * (NX * NC) + dp % (NX * NC)) * seqs + i % seqs
        pick = jnp.where(slot_ref[...] == wanted, 1.0, 0.0).astype(BF16)
        got = dot(pick[:, :rows], near_ref[...]) + dot(pick[:, rows:], far_ref[...])
        got = got.astype(BF16)
        for z in range(NZ):
            out_ref[z] = got[z * seqs : (z + 1) * seqs]

    return pl.pallas_call(
        body,
        out_shape=jax.ShapeDtypeStruct((NZ, seqs, width), BF16),
        in_specs=[vmem()] * (3 + len(ready)),
        out_specs=vmem(),
        compiler_params=SMALL,
    )(near, far, slot_here, *ready)


def fetch(after, array):
    def body(_, array_ref, out_ref):
        out_ref[...] = array_ref[...]

    return pl.pallas_call(
        body,
        out_shape=jax.ShapeDtypeStruct(array.shape, array.dtype),
        in_specs=[hbm(), vmem()],
        out_specs=vmem(),
        compiler_params=SMALL,
    )(after, array)


def absorb(arrived, w_uk, rope_part):
    _, seqs, width = arrived.shape
    heads, nope_dim, lat_part = w_uk.shape
    nope_width = heads * nope_dim
    rope_dim = width // heads - nope_dim
    ranks = lax.axis_size("rank")
    group = heads // ranks

    def body(arrived_ref, w_ref, lat_ref, rope_ref, lat_rows):
        rank = lax.axis_index("rank")
        query = arrived_ref[0].astype(F32)
        for z in range(1, NZ):
            query = query + arrived_ref[z].astype(F32)
        for h in range(heads):
            turned = (h // group - rank + ranks) % ranks * group + h % group
            lat_rows[pl.ds(pl.multiple_of(turned * seqs, seqs), seqs), :] = dot(
                query[:, h * nope_dim : (h + 1) * nope_dim].astype(BF16), w_ref[h]
            )
        rope_width = heads * rope_dim
        i, j = iota((rope_width, 128), 0), iota((rope_width, 128), 1)
        fold = (i % rope_dim - rank * rope_part == j) & (j < rope_part)
        fold = jnp.where(fold, 1.0, 0.0).astype(BF16)
        t = iota((heads, rope_width), 0)
        own_head = (t // group + rank) % ranks * group + t % group
        mine = own_head == iota((heads, rope_width), 1) // rope_dim
        for s in range(seqs):
            rows = slice(s * heads, (s + 1) * heads)
            lat_ref[rows, :] = lat_rows[pl.ds(s, heads, stride=seqs), :].astype(BF16)
            flat = jnp.broadcast_to(query[s : s + 1, nope_width:], (heads, rope_width))
            rope_ref[rows, :] = dot(jnp.where(mine, flat, 0.0).astype(BF16), fold).astype(BF16)

    return pl.pallas_call(
        body,
        out_shape=[
            jax.ShapeDtypeStruct((seqs * heads, lat_part), BF16),
            jax.ShapeDtypeStruct((seqs * heads, 128), BF16),
        ],
        in_specs=[vmem()] * 2,
        out_specs=[vmem()] * 2,
        compiler_params=SMALL,
        scratch_shapes=[pltpu.VMEM((heads * seqs, lat_part), F32)],
    )(arrived, w_uk)


def live_rows(bounds_ref, pos, slot):
    return (pos >= bounds_ref[slot : slot + 1, :1]) & (pos < bounds_ref[8 + slot : 9 + slot, :1])


def partial_scores(query_lat, query_rope, lengths, latent_cache, rope_keys, packed, scale):
    seqs, capacity, lat_part = latent_cache.shape
    heads = query_lat.shape[0] // seqs
    rope_part = rope_keys.shape[1]
    ranks = lax.axis_size("rank")
    group = heads // ranks
    blocks, half = packed // BLOCK, packed // BLOCK // 2

    def body(lat_ref, rope_ref, len_ref, cache_hbm, keys_hbm, *rest):
        outs, (bounds_ref, cache_ref, keys_ref, sems) = rest[:ranks], rest[ranks:]
        starts = [jnp.int32(0)]
        for s in range(seqs):
            starts.append(starts[-1] + (len_ref[s] + BLOCK - 1) // BLOCK)
        copies = []
        for b in range(blocks):
            slot = jnp.int32(0)
            start = jnp.int32(0)
            for s in range(1, seqs):
                slot = jnp.where(b >= starts[s], s, slot)
                start = jnp.where(b >= starts[s], starts[s], start)
            block = jnp.minimum(b - start, capacity // BLOCK - 1)
            source = pl.ds(pl.multiple_of(block * BLOCK, BLOCK), BLOCK)
            at = pl.ds(b * BLOCK, BLOCK)
            copies += [
                pltpu.make_async_copy(cache_hbm.at[slot, source], cache_ref.at[at], sems.at[0, b]),
                pltpu.make_async_copy(
                    keys_hbm.at[slot, :, source], keys_ref.at[:, at], sems.at[1, b]
                ),
            ]
            copies[-2].start()
            copies[-1].start()
        for s in range(seqs):
            first = starts[s] * BLOCK
            bounds_ref[s : s + 1, :] = jnp.full((1, 128), first, jnp.int32)
            bounds_ref[8 + s : 9 + s, :] = jnp.full((1, 128), first + len_ref[s], jnp.int32)
        lat, rope = lat_ref[...], rope_ref[:, :rope_part]
        for b in range(blocks):
            copies[2 * b].wait()
            copies[2 * b + 1].wait()
            at = pl.ds(b * BLOCK, BLOCK)
            every = lax.dot_general(
                lat, cache_ref[at, :], (((1,), (1,)), ((), ())), preferred_element_type=F32
            )
            every = every + dot(rope, keys_ref[:, at])
            part = every[:heads]
            for s in range(1, seqs):
                part = jnp.where(b >= starts[s], every[s * heads : (s + 1) * heads], part)
            part = part * scale
            row, to = b // half * group, pl.ds(b % half * BLOCK, BLOCK)
            for k in range(ranks):
                outs[k][row : row + group, to] = part[k * group : (k + 1) * group]

    return pl.pallas_call(
        body,
        out_shape=[jax.ShapeDtypeStruct((2 * group, packed // 2), F32)] * ranks
        + [
            jax.ShapeDtypeStruct((16, 128), jnp.int32),
            jax.ShapeDtypeStruct((packed, lat_part), BF16),
        ],
        in_specs=[vmem(), vmem(), smem(), hbm(), hbm()],
        out_specs=[vmem()] * (ranks + 2),
        compiler_params=SMALL,
        scratch_shapes=[
            pltpu.VMEM((rope_part, packed), BF16),
            pltpu.SemaphoreType.DMA((2, blocks)),
        ],
    )(query_lat, query_rope, lengths, latent_cache, rope_keys)


def softmax(parts, bounds, seqs):
    rows, width = parts[0].shape

    def body(*refs):
        *part_refs, bounds_ref, out_ref = refs
        total = part_refs[0][...]
        for ref in part_refs[1:]:
            total = total + ref[...]
        pos = iota((rows, width), 1) + iota((rows, width), 0) // (rows // 2) * width
        live = [live_rows(bounds_ref, pos, s) for s in range(seqs)]
        top = jnp.full((rows, width), jnp.inf, F32)
        for s in range(seqs):
            most = jnp.max(jnp.where(live[s], total, -jnp.inf), axis=1, keepdims=True)
            most = jnp.maximum(most, jnp.concatenate([most[rows // 2 :], most[: rows // 2]], axis=0))
            top = jnp.where(live[s], most, top)
        raised = jnp.exp(jnp.where(top < jnp.inf, total - top, -jnp.inf))
        below = jnp.ones((rows, width), F32)
        for s in range(seqs):
            sums = jnp.sum(jnp.where(live[s], raised, 0.0), axis=1, keepdims=True)
            sums = sums + jnp.concatenate([sums[rows // 2 :], sums[: rows // 2]], axis=0)
            below = jnp.where(live[s], sums, below)
        out_ref[...] = (raised / below).astype(BF16)

    return pl.pallas_call(
        body,
        out_shape=jax.ShapeDtypeStruct((rows, width), BF16),
        in_specs=[vmem()] * (len(parts) + 1),
        out_specs=vmem(),
        compiler_params=SMALL,
    )(*parts, bounds)


def head_part(weights, bounds, cache, w_uv, packed, seqs):
    heads, lat_part, value_dim = w_uv.shape
    ranks = len(weights)
    group = heads // ranks
    blocks, half = packed // BLOCK, packed // BLOCK // 2

    def body(*refs):
        weight_refs = refs[:ranks]
        bounds_ref, cache_ref, w_ref, out_ref, lat_rows = refs[ranks:]
        rank = lax.axis_index("rank")
        total = jnp.zeros((seqs * heads, lat_part), F32)
        for b in range(blocks):
            row, source = b // half * group, pl.ds(b % half * BLOCK, BLOCK)
            block = jnp.concatenate(
                [ref[:, source].astype(F32)[row : row + group] for ref in weight_refs], axis=0
            )
            pos = iota((heads, BLOCK), 1) + b * BLOCK
            block = jnp.concatenate(
                [
                    jnp.where(live_rows(bounds_ref, pos, s), block, 0.0).astype(BF16)
                    for s in range(seqs)
                ],
                axis=0,
            )
            total = total + dot(block, cache_ref[pl.ds(b * BLOCK, BLOCK), :])
        lat_rows[...] = total
        for k in range(ranks):
            for i in range(group):
                lat = lat_rows[pl.ds(k * group + i, seqs, stride=heads), :].astype(BF16)
                head = (rank - k + ranks) % ranks * group + i
                out_ref[:, pl.ds(pl.multiple_of(head * value_dim, value_dim), value_dim)] = dot(
                    lat, w_ref[head]
                ).astype(BF16)

    return pl.pallas_call(
        body,
        out_shape=jax.ShapeDtypeStruct((seqs, heads * value_dim), BF16),
        in_specs=[vmem()] * (ranks + 3),
        out_specs=vmem(),
        compiler_params=SMALL,
        scratch_shapes=[pltpu.VMEM((seqs * heads, lat_part), F32)],
    )(*weights, bounds, cache, w_uv)


def project(parts, w_out, copies):
    seqs = parts[0].shape[0]
    width = w_out.shape[1]

    def body(*refs):
        *part_refs, w_ref, out_ref = refs
        total = part_refs[0][...].astype(F32)
        for ref in part_refs[1:]:
            total = total + ref[...].astype(F32)
        out = dot(total.astype(BF16), w_ref[...]).astype(BF16)
        for d in range(copies):
            out_ref[d] = out

    return pl.pallas_call(
        body,
        out_shape=jax.ShapeDtypeStruct((copies, seqs, width), BF16),
        in_specs=[vmem()] * (len(parts) + 1),
        out_specs=vmem(),
        compiler_params=SMALL,
    )(*parts, w_out)


def bring_back(everyone, targets):
    devices, seqs, width = everyone.shape

    def body(all_ref, target_ref, out_ref):
        row = iota((seqs, width), 0)
        wanted = [jnp.broadcast_to(target_ref[j : j + 1, :], (seqs, width)) for j in range(seqs)]
        lines = [jnp.zeros((seqs, width), F32) for _ in range(seqs)]
        for d in range(devices):
            block = all_ref[d].astype(F32)
            for j in range(seqs):
                lines[j] = jnp.where(wanted[j] == row + d * seqs, block, lines[j])
        for j in range(seqs):
            mine = wanted[j] % seqs == row
            line = jnp.sum(jnp.where(mine, lines[j], 0.0), axis=0, keepdims=True)
            out_ref[j : j + 1, :] = line.astype(BF16)

    return pl.pallas_call(
        body,
        out_shape=jax.ShapeDtypeStruct((seqs, width), BF16),
        in_specs=[vmem()] * 2,
        out_specs=vmem(),
        compiler_params=SMALL,
    )(everyone, targets)


def per_device(q_nope, q_rope, latent_cache, rope_keys, lengths, slot_of, w_uk, w_uv, w_out):
    seqs = q_nope.shape[0]
    heads, nope_dim, _ = w_uk.shape
    scale = 1.0 / math.sqrt(nope_dim + q_rope.shape[1] // heads)
    seq_total = slot_of.shape[0]
    ranks = lax.axis_size("rank")
    z_groups, x_groups, c_groups = dp_groups()

    dp_pos = lax.axis_index("dp")
    plane_rows = 2 * NX * seqs
    at = jnp.arange(plane_rows, dtype=jnp.int32)
    from_c = (dp_pos % NC + at // (NX * seqs)) % NC
    from_x = (dp_pos // NC % NX + NX - at // seqs % NX) % NX
    row_of = ((dp_pos // (NC * NX) * NX + from_x) * NC + from_c) * seqs + at % seqs
    slot_here = jnp.sum(
        jnp.where(
            row_of[:, None] == jnp.arange(seq_total, dtype=jnp.int32)[None, :], slot_of[None, :], 0
        ),
        axis=1,
    ).reshape(1, plane_rows)

    targets = lax.dynamic_slice_in_dim(slot_of, dp_pos * seqs, seqs).reshape(seqs, 1)

    sizes = [n for n in SIZES if n < seqs * latent_cache.shape[1]] + [seqs * latent_cache.shape[1]]
    needed = jnp.sum((lengths + BLOCK - 1) // BLOCK) * BLOCK
    which = sum((needed > n).astype(jnp.int32) for n in sizes[:-1])

    rows = join(q_nope, q_rope)
    near = [rows] + [shifted(rows, "dp", x_groups, k) for k in range(1, NX)]
    near = jnp.concatenate(near, axis=0)
    far = shifted(near, "dp", c_groups, 1)
    picked = pick_rows(near, far, slot_here, seqs, (targets, which.reshape(1, 1)))
    arrived = lax.all_to_all(picked, "dp", 0, 0, axis_index_groups=z_groups, tiled=True)

    query_lat, query_rope = absorb(arrived, fetch(picked, w_uk), rope_keys.shape[1])

    def attend(packed):
        def branch(query_lat, query_rope, lengths, latent_cache, rope_keys, w_uv):
            own, *others, bounds, held = partial_scores(
                query_lat, query_rope, lengths, latent_cache, rope_keys, packed, scale
            )
            weights = softmax([own] + from_ranks(others), bounds, seqs)
            gathered = [weights] + from_ranks([weights] * (ranks - 1))
            return head_part(gathered, bounds, held, w_uv, packed, seqs)

        return branch

    value_part = lax.switch(
        which,
        [attend(n) for n in sizes],
        query_lat,
        query_rope,
        lengths,
        latent_cache,
        rope_keys,
        w_uv,
    )
    parts = [value_part] + from_ranks([value_part] * (ranks - 1))
    copies = project(parts, w_out, lax.axis_size("dp"))
    everyone = lax.all_to_all(copies, "dp", 0, 0, tiled=True)
    return bring_back(everyone, targets)


def solution(mesh):
    placed = (
        P("dp", None),
        P("dp", None),
        P("dp", None, "rank"),
        P("dp", "rank", None),
        P("dp"),
        P(),
        P(None, None, "rank"),
        P(None, "rank", None),
        P(None, "rank"),
    )
    return jax.shard_map(
        per_device, mesh=mesh, in_specs=placed, out_specs=P("dp", "rank"), check_vma=False
    )
```

```python
import math

import jax
import jax.numpy as jnp
from jax import lax
from jax.experimental import pallas as pl
from jax.experimental.pallas import tpu as pltpu
from jax.sharding import PartitionSpec as P

NZ, NX, NC = 8, 4, 2


def dp_groups():
    z_groups = [[z * NX * NC + p for z in range(NZ)] for p in range(NX * NC)]
    x_groups = [[(z * NX + x) * NC + c for x in range(NX)] for z in range(NZ) for c in range(NC)]
    c_groups = [[i * NC + c for c in range(NC)] for i in range(NZ * NX)]
    return z_groups, x_groups, c_groups


def shifted(array, axis, groups, step):
    pairs = [(g[i], g[(i + step) % len(g)]) for g in groups for i in range(len(g))]
    return lax.ppermute(array, axis, pairs)


def from_ranks(arrays):
    ring = [list(range(lax.axis_size("rank")))]
    return [shifted(a, "rank", ring, k) for k, a in enumerate(arrays, start=1)]


def placed_as(order, arrays):
    return [arrays[k] for k in order]


F32, BF16 = jnp.float32, jnp.bfloat16
BLOCK = 512
FIRST_FAR, LAST_FAR = (0, 2, 1, 3), (0, 3, 1, 2)
SIZES = (9216, 10240, 12288)
SMALL = pltpu.CompilerParams(vmem_limit_bytes=8 << 20)
SCORES = pltpu.CompilerParams(vmem_limit_bytes=16 << 20)


def vmem():
    return pl.BlockSpec(memory_space=pltpu.VMEM)


def smem():
    return pl.BlockSpec(memory_space=pltpu.SMEM)


def hbm():
    return pl.BlockSpec(memory_space=pltpu.HBM)


def dot(a, b):
    return jnp.dot(a, b, preferred_element_type=F32)


def iota(shape, dim):
    return lax.broadcasted_iota(jnp.int32, shape, dim)


def join(q_nope, q_rope):
    seqs, nope_width = q_nope.shape
    width = nope_width + q_rope.shape[1]

    def body(nope_ref, rope_ref, out_ref, sems):
        copies = [
            pltpu.make_async_copy(nope_ref, out_ref.at[:, :nope_width], sems.at[0]),
            pltpu.make_async_copy(rope_ref, out_ref.at[:, nope_width:], sems.at[1]),
        ]
        for copy in copies:
            copy.start()
        for copy in copies:
            copy.wait()

    return pl.pallas_call(
        body,
        out_shape=jax.ShapeDtypeStruct((seqs, width), BF16),
        in_specs=[hbm()] * 2,
        out_specs=vmem(),
        scratch_shapes=[pltpu.SemaphoreType.DMA((2,))],
        compiler_params=SMALL,
    )(q_nope, q_rope)


def pick_rows(near, far, slot_here, seqs, ready):
    rows, width = near.shape

    def body(near_ref, far_ref, slot_ref, *rest):
        out_ref = rest[-1]
        dp = lax.axis_index("dp")
        i = iota((NZ * seqs, 2 * rows), 0)
        wanted = (i // seqs * (NX * NC) + dp % (NX * NC)) * seqs + i % seqs
        pick = jnp.where(slot_ref[...] == wanted, 1.0, 0.0).astype(BF16)
        got = dot(pick[:, :rows], near_ref[...]) + dot(pick[:, rows:], far_ref[...])
        got = got.astype(BF16)
        for z in range(NZ):
            out_ref[z] = got[z * seqs : (z + 1) * seqs]

    return pl.pallas_call(
        body,
        out_shape=jax.ShapeDtypeStruct((NZ, seqs, width), BF16),
        in_specs=[vmem()] * (3 + len(ready)),
        out_specs=vmem(),
        compiler_params=SMALL,
    )(near, far, slot_here, *ready)


def fetch(after, array):
    def body(_, array_ref, out_ref):
        out_ref[...] = array_ref[...]

    return pl.pallas_call(
        body,
        out_shape=jax.ShapeDtypeStruct(array.shape, array.dtype),
        in_specs=[hbm(), vmem()],
        out_specs=vmem(),
        compiler_params=SMALL,
    )(after, array)


def absorb(arrived, w_uk, rope_part):
    _, seqs, width = arrived.shape
    heads, nope_dim, lat_part = w_uk.shape
    nope_width = heads * nope_dim
    rope_dim = width // heads - nope_dim
    ranks = lax.axis_size("rank")
    group = heads // ranks

    def body(arrived_ref, w_ref, lat_ref, rope_ref, lat_rows):
        rank = lax.axis_index("rank")
        query = arrived_ref[0].astype(F32)
        for z in range(1, NZ):
            query = query + arrived_ref[z].astype(F32)
        for h in range(heads):
            turned = (h // group - rank + ranks) % ranks * group + h % group
            lat_rows[pl.ds(pl.multiple_of(turned * seqs, seqs), seqs), :] = dot(
                query[:, h * nope_dim : (h + 1) * nope_dim].astype(BF16), w_ref[h]
            )
        rope_width = heads * rope_dim
        i, j = iota((rope_width, 128), 0), iota((rope_width, 128), 1)
        fold = (i % rope_dim - rank * rope_part == j) & (j < rope_part)
        fold = jnp.where(fold, 1.0, 0.0).astype(BF16)
        t = iota((heads, rope_width), 0)
        own_head = (t // group + rank) % ranks * group + t % group
        mine = own_head == iota((heads, rope_width), 1) // rope_dim
        for s in range(seqs):
            rows = slice(s * heads, (s + 1) * heads)
            lat_ref[rows, :] = lat_rows[pl.ds(s, heads, stride=seqs), :].astype(BF16)
            flat = jnp.broadcast_to(query[s : s + 1, nope_width:], (heads, rope_width))
            rope_ref[rows, :] = dot(jnp.where(mine, flat, 0.0).astype(BF16), fold).astype(BF16)

    return pl.pallas_call(
        body,
        out_shape=[
            jax.ShapeDtypeStruct((seqs * heads, lat_part), BF16),
            jax.ShapeDtypeStruct((seqs * heads, 128), BF16),
        ],
        in_specs=[vmem()] * 2,
        out_specs=[vmem()] * 2,
        compiler_params=SMALL,
        scratch_shapes=[pltpu.VMEM((heads * seqs, lat_part), F32)],
    )(arrived, w_uk)


def live_rows(bounds_ref, pos, slot):
    return (pos >= bounds_ref[slot : slot + 1, :1]) & (pos < bounds_ref[8 + slot : 9 + slot, :1])


def partial_scores(query_lat, query_rope, lengths, latent_cache, rope_keys, packed, scale):
    seqs, capacity, lat_part = latent_cache.shape
    heads = query_lat.shape[0] // seqs
    rope_part = rope_keys.shape[1]
    ranks = lax.axis_size("rank")
    group = heads // ranks
    blocks, half = packed // BLOCK, packed // BLOCK // 2

    def body(lat_ref, rope_ref, len_ref, cache_hbm, keys_hbm, *rest):
        outs, (bounds_ref, packed_ref, cache_ref, keys_ref, sems) = rest[:ranks], rest[ranks:]
        copies = [pltpu.make_async_copy(keys_hbm, keys_ref, sems.at[seqs])]
        for s in range(seqs):
            copies.append(pltpu.make_async_copy(cache_hbm.at[s], cache_ref.at[s], sems.at[s]))
        for copy in copies:
            copy.start()
        starts = [jnp.int32(0)]
        for s in range(seqs):
            starts.append(starts[-1] + (len_ref[s] + BLOCK - 1) // BLOCK)
        for s in range(seqs):
            first = starts[s] * BLOCK
            bounds_ref[s : s + 1, :] = jnp.full((1, 128), first, jnp.int32)
            bounds_ref[8 + s : 9 + s, :] = jnp.full((1, 128), first + len_ref[s], jnp.int32)
        lat, rope = lat_ref[...], rope_ref[:, :rope_part]
        for copy in copies:
            copy.wait()
        for b in range(blocks):
            slot = jnp.int32(0)
            start = jnp.int32(0)
            for s in range(1, seqs):
                slot = jnp.where(b >= starts[s], s, slot)
                start = jnp.where(b >= starts[s], starts[s], start)
            block = jnp.minimum(b - start, capacity // BLOCK - 1)
            source = pl.ds(pl.multiple_of(block * BLOCK, BLOCK), BLOCK)
            rows = cache_ref[slot, source, :]
            packed_ref[b * BLOCK : (b + 1) * BLOCK, :] = rows
            every = lax.dot_general(
                lat, rows, (((1,), (1,)), ((), ())), preferred_element_type=F32
            )
            every = every + dot(rope, keys_ref[slot, :, source])
            part = every[:heads]
            for s in range(1, seqs):
                part = jnp.where(b >= starts[s], every[s * heads : (s + 1) * heads], part)
            part = part * scale
            row, to = b // half * group, pl.ds(b % half * BLOCK, BLOCK)
            for k in range(ranks):
                outs[k][row : row + group, to] = part[k * group : (k + 1) * group]

    return pl.pallas_call(
        body,
        out_shape=[jax.ShapeDtypeStruct((2 * group, packed // 2), F32)] * ranks
        + [
            jax.ShapeDtypeStruct((16, 128), jnp.int32),
            jax.ShapeDtypeStruct((packed, lat_part), BF16),
        ],
        in_specs=[vmem(), vmem(), smem(), hbm(), hbm()],
        out_specs=[vmem()] * (ranks + 2),
        compiler_params=SCORES,
        scratch_shapes=[
            pltpu.VMEM(latent_cache.shape, BF16),
            pltpu.VMEM(rope_keys.shape, BF16),
            pltpu.SemaphoreType.DMA((seqs + 1,)),
        ],
    )(query_lat, query_rope, lengths, latent_cache, rope_keys)


def softmax(parts, bounds, seqs):
    rows, width = parts[0].shape

    def body(*refs):
        *part_refs, bounds_ref, out_ref = refs
        total = part_refs[0][...]
        for ref in part_refs[1:]:
            total = total + ref[...]
        pos = iota((rows, width), 1) + iota((rows, width), 0) // (rows // 2) * width
        live = [live_rows(bounds_ref, pos, s) for s in range(seqs)]
        top = jnp.full((rows, width), jnp.inf, F32)
        for s in range(seqs):
            most = jnp.max(jnp.where(live[s], total, -jnp.inf), axis=1, keepdims=True)
            most = jnp.maximum(most, jnp.concatenate([most[rows // 2 :], most[: rows // 2]], axis=0))
            top = jnp.where(live[s], most, top)
        raised = jnp.exp(jnp.where(top < jnp.inf, total - top, -jnp.inf))
        below = jnp.ones((rows, width), F32)
        for s in range(seqs):
            sums = jnp.sum(jnp.where(live[s], raised, 0.0), axis=1, keepdims=True)
            sums = sums + jnp.concatenate([sums[rows // 2 :], sums[: rows // 2]], axis=0)
            below = jnp.where(live[s], sums, below)
        out_ref[...] = (raised / below).astype(BF16)

    return pl.pallas_call(
        body,
        out_shape=jax.ShapeDtypeStruct((rows, width), BF16),
        in_specs=[vmem()] * (len(parts) + 1),
        out_specs=vmem(),
        compiler_params=SMALL,
    )(*parts, bounds)


def head_part(weights, bounds, cache, w_uv, packed, seqs):
    heads, lat_part, value_dim = w_uv.shape
    ranks = len(weights)
    group = heads // ranks
    blocks, half = packed // BLOCK, packed // BLOCK // 2

    def body(*refs):
        weight_refs = [refs[LAST_FAR.index(k)] for k in range(ranks)]
        bounds_ref, cache_ref, w_ref, out_ref, lat_rows = refs[ranks:]
        rank = lax.axis_index("rank")
        total = jnp.zeros((seqs * heads, lat_part), F32)
        for b in range(blocks):
            row, source = b // half * group, pl.ds(b % half * BLOCK, BLOCK)
            block = jnp.concatenate(
                [ref[:, source].astype(F32)[row : row + group] for ref in weight_refs], axis=0
            )
            pos = iota((heads, BLOCK), 1) + b * BLOCK
            block = jnp.concatenate(
                [
                    jnp.where(live_rows(bounds_ref, pos, s), block, 0.0).astype(BF16)
                    for s in range(seqs)
                ],
                axis=0,
            )
            total = total + dot(block, cache_ref[pl.ds(b * BLOCK, BLOCK), :])
        lat_rows[...] = total
        for k in range(ranks):
            for i in range(group):
                lat = lat_rows[pl.ds(k * group + i, seqs, stride=heads), :].astype(BF16)
                head = (rank - k + ranks) % ranks * group + i
                out_ref[:, pl.ds(pl.multiple_of(head * value_dim, value_dim), value_dim)] = dot(
                    lat, w_ref[head]
                ).astype(BF16)

    return pl.pallas_call(
        body,
        out_shape=jax.ShapeDtypeStruct((seqs, heads * value_dim), BF16),
        in_specs=[vmem()] * (ranks + 3),
        out_specs=vmem(),
        compiler_params=SMALL,
        scratch_shapes=[pltpu.VMEM((seqs * heads, lat_part), F32)],
    )(*placed_as(LAST_FAR, weights), bounds, cache, w_uv)


def project(parts, w_out, copies):
    seqs = parts[0].shape[0]
    width = w_out.shape[1]

    def body(*refs):
        *part_refs, w_ref, out_ref = refs
        total = part_refs[0][...].astype(F32)
        for ref in part_refs[1:]:
            total = total + ref[...].astype(F32)
        out = dot(total.astype(BF16), w_ref[...]).astype(BF16)
        for d in range(copies):
            out_ref[d] = out

    return pl.pallas_call(
        body,
        out_shape=jax.ShapeDtypeStruct((copies, seqs, width), BF16),
        in_specs=[vmem()] * (len(parts) + 1),
        out_specs=vmem(),
        compiler_params=SMALL,
    )(*parts, w_out)


def bring_back(everyone, targets):
    devices, seqs, width = everyone.shape

    def body(all_ref, target_ref, out_ref):
        row = iota((seqs, width), 0)
        wanted = [jnp.broadcast_to(target_ref[j : j + 1, :], (seqs, width)) for j in range(seqs)]
        lines = [jnp.zeros((seqs, width), F32) for _ in range(seqs)]
        for d in range(devices):
            block = all_ref[d].astype(F32)
            for j in range(seqs):
                lines[j] = jnp.where(wanted[j] == row + d * seqs, block, lines[j])
        for j in range(seqs):
            mine = wanted[j] % seqs == row
            line = jnp.sum(jnp.where(mine, lines[j], 0.0), axis=0, keepdims=True)
            out_ref[j : j + 1, :] = line.astype(BF16)

    return pl.pallas_call(
        body,
        out_shape=jax.ShapeDtypeStruct((seqs, width), BF16),
        in_specs=[vmem()] * 2,
        out_specs=vmem(),
        compiler_params=SMALL,
    )(everyone, targets)


def per_device(q_nope, q_rope, latent_cache, rope_keys, lengths, slot_of, w_uk, w_uv, w_out):
    seqs = q_nope.shape[0]
    heads, nope_dim, _ = w_uk.shape
    scale = 1.0 / math.sqrt(nope_dim + q_rope.shape[1] // heads)
    seq_total = slot_of.shape[0]
    ranks = lax.axis_size("rank")
    z_groups, x_groups, c_groups = dp_groups()

    dp_pos = lax.axis_index("dp")
    plane_rows = 2 * NX * seqs
    at = jnp.arange(plane_rows, dtype=jnp.int32)
    from_c = (dp_pos % NC + at // (NX * seqs)) % NC
    from_x = (dp_pos // NC % NX + NX - at // seqs % NX) % NX
    row_of = ((dp_pos // (NC * NX) * NX + from_x) * NC + from_c) * seqs + at % seqs
    slot_here = jnp.sum(
        jnp.where(
            row_of[:, None] == jnp.arange(seq_total, dtype=jnp.int32)[None, :], slot_of[None, :], 0
        ),
        axis=1,
    ).reshape(1, plane_rows)

    targets = lax.dynamic_slice_in_dim(slot_of, dp_pos * seqs, seqs).reshape(seqs, 1)

    sizes = [n for n in SIZES if n < seqs * latent_cache.shape[1]] + [seqs * latent_cache.shape[1]]
    needed = jnp.sum((lengths + BLOCK - 1) // BLOCK) * BLOCK
    which = sum((needed > n).astype(jnp.int32) for n in sizes[:-1])

    rows = join(q_nope, q_rope)
    near = [rows] + [shifted(rows, "dp", x_groups, k) for k in range(1, NX)]
    near = jnp.concatenate(near, axis=0)
    far = shifted(near, "dp", c_groups, 1)
    picked = pick_rows(near, far, slot_here, seqs, (targets, which.reshape(1, 1)))
    arrived = lax.all_to_all(picked, "dp", 0, 0, axis_index_groups=z_groups, tiled=True)

    query_lat, query_rope = absorb(arrived, fetch(picked, w_uk), rope_keys.shape[1])

    def attend(packed):
        def branch(query_lat, query_rope, lengths, latent_cache, rope_keys, w_uv):
            own, *others, bounds, held = partial_scores(
                query_lat, query_rope, lengths, latent_cache, rope_keys, packed, scale
            )
            parts = placed_as(FIRST_FAR, [own] + from_ranks(others))
            weights = softmax(parts, bounds, seqs)
            gathered = [weights] + from_ranks([weights] * (ranks - 1))
            return head_part(gathered, bounds, held, w_uv, packed, seqs)

        return branch

    value_part = lax.switch(
        which,
        [attend(n) for n in sizes],
        query_lat,
        query_rope,
        lengths,
        latent_cache,
        rope_keys,
        w_uv,
    )
    parts = [value_part] + from_ranks([value_part] * (ranks - 1))
    copies = project(placed_as(LAST_FAR, parts), w_out, lax.axis_size("dp"))
    everyone = lax.all_to_all(copies, "dp", 0, 0, tiled=True)
    return bring_back(everyone, targets)


def solution(mesh):
    placed = (
        P("dp", None),
        P("dp", None),
        P("dp", None, "rank"),
        P("dp", "rank", None),
        P("dp"),
        P(),
        P(None, None, "rank"),
        P(None, "rank", None),
        P(None, "rank"),
    )
    return jax.shard_map(
        per_device, mesh=mesh, in_specs=placed, out_specs=P("dp", "rank"), check_vma=False
    )
```

```python
import math

import jax
import jax.numpy as jnp
from jax import lax
from jax.experimental import pallas as pl
from jax.experimental.pallas import tpu as pltpu
from jax.sharding import PartitionSpec as P

NZ, NX, NC = 8, 4, 2


def dp_groups():
    z_groups = [[z * NX * NC + p for z in range(NZ)] for p in range(NX * NC)]
    x_groups = [[(z * NX + x) * NC + c for x in range(NX)] for z in range(NZ) for c in range(NC)]
    c_groups = [[i * NC + c for c in range(NC)] for i in range(NZ * NX)]
    return z_groups, x_groups, c_groups


def shifted(array, axis, groups, step):
    pairs = [(g[i], g[(i + step) % len(g)]) for g in groups for i in range(len(g))]
    return lax.ppermute(array, axis, pairs)


def from_ranks(arrays):
    ring = [list(range(lax.axis_size("rank")))]
    return [shifted(a, "rank", ring, k) for k, a in enumerate(arrays, start=1)]


def placed_as(order, arrays):
    return [arrays[k] for k in order]


F32, BF16 = jnp.float32, jnp.bfloat16
BLOCK = 512
FIRST_FAR, LAST_FAR = (0, 2, 1, 3), (0, 3, 1, 2)
SIZES = (9216, 10240, 12288)
SMALL = pltpu.CompilerParams(vmem_limit_bytes=8 << 20)
SCORES = pltpu.CompilerParams(vmem_limit_bytes=16 << 20)


def vmem():
    return pl.BlockSpec(memory_space=pltpu.VMEM)


def hbm():
    return pl.BlockSpec(memory_space=pltpu.HBM)


def dot(a, b):
    return jnp.dot(a, b, preferred_element_type=F32)


def iota(shape, dim):
    return lax.broadcasted_iota(jnp.int32, shape, dim)


def join(q_nope, q_rope):
    seqs, nope_width = q_nope.shape
    width = nope_width + q_rope.shape[1]

    def body(nope_ref, rope_ref, out_ref, sems):
        copies = [
            pltpu.make_async_copy(nope_ref, out_ref.at[:, :nope_width], sems.at[0]),
            pltpu.make_async_copy(rope_ref, out_ref.at[:, nope_width:], sems.at[1]),
        ]
        for copy in copies:
            copy.start()
        for copy in copies:
            copy.wait()

    return pl.pallas_call(
        body,
        out_shape=jax.ShapeDtypeStruct((seqs, width), BF16),
        in_specs=[hbm()] * 2,
        out_specs=vmem(),
        scratch_shapes=[pltpu.SemaphoreType.DMA((2,))],
        compiler_params=SMALL,
    )(q_nope, q_rope)


def pick_rows(near, far, slot_here, seqs, ready):
    rows, width = near.shape

    def body(near_ref, far_ref, slot_ref, *rest):
        out_ref = rest[-1]
        dp = lax.axis_index("dp")
        i = iota((NZ * seqs, 2 * rows), 0)
        wanted = (i // seqs * (NX * NC) + dp % (NX * NC)) * seqs + i % seqs
        pick = jnp.where(slot_ref[...] == wanted, 1.0, 0.0).astype(BF16)
        got = dot(pick[:, :rows], near_ref[...]) + dot(pick[:, rows:], far_ref[...])
        got = got.astype(BF16)
        for z in range(NZ):
            out_ref[z] = got[z * seqs : (z + 1) * seqs]

    return pl.pallas_call(
        body,
        out_shape=jax.ShapeDtypeStruct((NZ, seqs, width), BF16),
        in_specs=[vmem()] * (3 + len(ready)),
        out_specs=vmem(),
        compiler_params=SMALL,
    )(near, far, slot_here, *ready)


def fetch(after, array):
    def body(_, array_ref, out_ref):
        out_ref[...] = array_ref[...]

    return pl.pallas_call(
        body,
        out_shape=jax.ShapeDtypeStruct(array.shape, array.dtype),
        in_specs=[hbm(), vmem()],
        out_specs=vmem(),
        compiler_params=SMALL,
    )(after, array)


def absorb(arrived, w_uk, rope_part):
    _, seqs, width = arrived.shape
    heads, nope_dim, lat_part = w_uk.shape
    nope_width = heads * nope_dim
    rope_dim = width // heads - nope_dim
    ranks = lax.axis_size("rank")
    group = heads // ranks

    def body(arrived_ref, w_ref, lat_ref, rope_ref, lat_rows):
        rank = lax.axis_index("rank")
        query = arrived_ref[0].astype(F32)
        for z in range(1, NZ):
            query = query + arrived_ref[z].astype(F32)
        for h in range(heads):
            turned = (h // group - rank + ranks) % ranks * group + h % group
            lat_rows[pl.ds(pl.multiple_of(turned * seqs, seqs), seqs), :] = dot(
                query[:, h * nope_dim : (h + 1) * nope_dim].astype(BF16), w_ref[h]
            )
        rope_width = heads * rope_dim
        i, j = iota((rope_width, 128), 0), iota((rope_width, 128), 1)
        fold = (i % rope_dim - rank * rope_part == j) & (j < rope_part)
        fold = jnp.where(fold, 1.0, 0.0).astype(BF16)
        t = iota((heads, rope_width), 0)
        own_head = (t // group + rank) % ranks * group + t % group
        mine = own_head == iota((heads, rope_width), 1) // rope_dim
        for s in range(seqs):
            rows = slice(s * heads, (s + 1) * heads)
            lat_ref[rows, :] = lat_rows[pl.ds(s, heads, stride=seqs), :].astype(BF16)
            flat = jnp.broadcast_to(query[s : s + 1, nope_width:], (heads, rope_width))
            rope_ref[rows, :] = dot(jnp.where(mine, flat, 0.0).astype(BF16), fold).astype(BF16)

    return pl.pallas_call(
        body,
        out_shape=[
            jax.ShapeDtypeStruct((seqs * heads, lat_part), BF16),
            jax.ShapeDtypeStruct((seqs * heads, 128), BF16),
        ],
        in_specs=[vmem()] * 2,
        out_specs=[vmem()] * 2,
        compiler_params=SMALL,
        scratch_shapes=[pltpu.VMEM((heads * seqs, lat_part), F32)],
    )(arrived, w_uk)


def live_rows(bounds_ref, pos, slot):
    return (pos >= bounds_ref[slot : slot + 1, :1]) & (pos < bounds_ref[8 + slot : 9 + slot, :1])


def partial_scores(query_lat, query_rope, lengths, latent_cache, rope_keys, packed, scale):
    seqs, capacity, lat_part = latent_cache.shape
    heads = query_lat.shape[0] // seqs
    rope_part = rope_keys.shape[1]
    ranks = lax.axis_size("rank")
    group = heads // ranks
    blocks, half = packed // BLOCK, packed // BLOCK // 2

    def body(lat_ref, rope_ref, len_hbm, cache_hbm, keys_hbm, *rest):
        outs, rest = rest[:ranks], rest[ranks:]
        bounds_ref, packed_ref, cache_ref, keys_ref, len_ref, sems = rest
        copies = [pltpu.make_async_copy(keys_hbm, keys_ref, sems.at[seqs])]
        for s in range(seqs):
            copies.append(pltpu.make_async_copy(cache_hbm.at[s], cache_ref.at[s], sems.at[s]))
        for copy in copies:
            copy.start()
        lengths_copy = pltpu.make_async_copy(len_hbm, len_ref, sems.at[seqs + 1])
        lengths_copy.start()
        lengths_copy.wait()
        starts = [jnp.int32(0)]
        for s in range(seqs):
            starts.append(starts[-1] + (len_ref[s] + BLOCK - 1) // BLOCK)
        for s in range(seqs):
            first = starts[s] * BLOCK
            bounds_ref[s : s + 1, :] = jnp.full((1, 128), first, jnp.int32)
            bounds_ref[8 + s : 9 + s, :] = jnp.full((1, 128), first + len_ref[s], jnp.int32)
        lat, rope = lat_ref[...], rope_ref[:, :rope_part]
        for copy in copies:
            copy.wait()
        for b in range(blocks):
            slot = jnp.int32(0)
            start = jnp.int32(0)
            for s in range(1, seqs):
                slot = jnp.where(b >= starts[s], s, slot)
                start = jnp.where(b >= starts[s], starts[s], start)
            block = jnp.minimum(b - start, capacity // BLOCK - 1)
            source = pl.ds(pl.multiple_of(block * BLOCK, BLOCK), BLOCK)
            rows = cache_ref[slot, source, :]
            packed_ref[b * BLOCK : (b + 1) * BLOCK, :] = rows
            every = lax.dot_general(
                lat, rows, (((1,), (1,)), ((), ())), preferred_element_type=F32
            )
            every = every + dot(rope, keys_ref[slot, :, source])
            part = every[:heads]
            for s in range(1, seqs):
                part = jnp.where(b >= starts[s], every[s * heads : (s + 1) * heads], part)
            part = part * scale
            row, to = b // half * group, pl.ds(b % half * BLOCK, BLOCK)
            for k in range(ranks):
                outs[k][row : row + group, to] = part[k * group : (k + 1) * group]

    return pl.pallas_call(
        body,
        out_shape=[jax.ShapeDtypeStruct((2 * group, packed // 2), F32)] * ranks
        + [
            jax.ShapeDtypeStruct((16, 128), jnp.int32),
            jax.ShapeDtypeStruct((packed, lat_part), BF16),
        ],
        in_specs=[vmem()] * 2 + [hbm()] * 3,
        out_specs=[vmem()] * (ranks + 2),
        compiler_params=SCORES,
        scratch_shapes=[
            pltpu.VMEM(latent_cache.shape, BF16),
            pltpu.VMEM(rope_keys.shape, BF16),
            pltpu.SMEM((seqs,), jnp.int32),
            pltpu.SemaphoreType.DMA((seqs + 2,)),
        ],
    )(query_lat, query_rope, lengths, latent_cache, rope_keys)


def softmax(parts, bounds, seqs):
    rows, width = parts[0].shape

    def body(*refs):
        *part_refs, bounds_ref, out_ref = refs
        total = part_refs[0][...]
        for ref in part_refs[1:]:
            total = total + ref[...]
        pos = iota((rows, width), 1) + iota((rows, width), 0) // (rows // 2) * width
        live = [live_rows(bounds_ref, pos, s) for s in range(seqs)]
        top = jnp.full((rows, width), jnp.inf, F32)
        for s in range(seqs):
            most = jnp.max(jnp.where(live[s], total, -jnp.inf), axis=1, keepdims=True)
            most = jnp.maximum(most, jnp.concatenate([most[rows // 2 :], most[: rows // 2]], axis=0))
            top = jnp.where(live[s], most, top)
        raised = jnp.exp(jnp.where(top < jnp.inf, total - top, -jnp.inf))
        below = jnp.ones((rows, width), F32)
        for s in range(seqs):
            sums = jnp.sum(jnp.where(live[s], raised, 0.0), axis=1, keepdims=True)
            sums = sums + jnp.concatenate([sums[rows // 2 :], sums[: rows // 2]], axis=0)
            below = jnp.where(live[s], sums, below)
        out_ref[...] = (raised / below).astype(BF16)

    return pl.pallas_call(
        body,
        out_shape=jax.ShapeDtypeStruct((rows, width), BF16),
        in_specs=[vmem()] * (len(parts) + 1),
        out_specs=vmem(),
        compiler_params=SMALL,
    )(*parts, bounds)


def head_part(weights, bounds, cache, w_uv, packed, seqs):
    heads, lat_part, value_dim = w_uv.shape
    ranks = len(weights)
    group = heads // ranks
    blocks, half = packed // BLOCK, packed // BLOCK // 2

    def body(*refs):
        weight_refs = [refs[LAST_FAR.index(k)] for k in range(ranks)]
        bounds_ref, cache_ref, w_ref, out_ref, lat_rows = refs[ranks:]
        rank = lax.axis_index("rank")
        total = jnp.zeros((seqs * heads, lat_part), F32)
        for b in range(blocks):
            row, source = b // half * group, pl.ds(b % half * BLOCK, BLOCK)
            block = jnp.concatenate(
                [ref[:, source].astype(F32)[row : row + group] for ref in weight_refs], axis=0
            )
            pos = iota((heads, BLOCK), 1) + b * BLOCK
            block = jnp.concatenate(
                [
                    jnp.where(live_rows(bounds_ref, pos, s), block, 0.0).astype(BF16)
                    for s in range(seqs)
                ],
                axis=0,
            )
            total = total + dot(block, cache_ref[pl.ds(b * BLOCK, BLOCK), :])
        lat_rows[...] = total
        for k in range(ranks):
            for i in range(group):
                lat = lat_rows[pl.ds(k * group + i, seqs, stride=heads), :].astype(BF16)
                head = (rank - k + ranks) % ranks * group + i
                out_ref[:, pl.ds(pl.multiple_of(head * value_dim, value_dim), value_dim)] = dot(
                    lat, w_ref[head]
                ).astype(BF16)

    return pl.pallas_call(
        body,
        out_shape=jax.ShapeDtypeStruct((seqs, heads * value_dim), BF16),
        in_specs=[vmem()] * (ranks + 3),
        out_specs=vmem(),
        compiler_params=SMALL,
        scratch_shapes=[pltpu.VMEM((seqs * heads, lat_part), F32)],
    )(*placed_as(LAST_FAR, weights), bounds, cache, w_uv)


def project(parts, w_out, copies):
    seqs = parts[0].shape[0]
    width = w_out.shape[1]

    def body(*refs):
        *part_refs, w_ref, out_ref = refs
        total = part_refs[0][...].astype(F32)
        for ref in part_refs[1:]:
            total = total + ref[...].astype(F32)
        out = dot(total.astype(BF16), w_ref[...]).astype(BF16)
        for d in range(copies):
            out_ref[d] = out

    return pl.pallas_call(
        body,
        out_shape=jax.ShapeDtypeStruct((copies, seqs, width), BF16),
        in_specs=[vmem()] * (len(parts) + 1),
        out_specs=vmem(),
        compiler_params=SMALL,
    )(*parts, w_out)


def bring_back(everyone, targets):
    devices, seqs, width = everyone.shape

    def body(all_ref, target_ref, out_ref):
        row = iota((seqs, width), 0)
        wanted = [jnp.broadcast_to(target_ref[j : j + 1, :], (seqs, width)) for j in range(seqs)]
        lines = [jnp.zeros((seqs, width), F32) for _ in range(seqs)]
        for d in range(devices):
            block = all_ref[d].astype(F32)
            for j in range(seqs):
                lines[j] = jnp.where(wanted[j] == row + d * seqs, block, lines[j])
        for j in range(seqs):
            mine = wanted[j] % seqs == row
            line = jnp.sum(jnp.where(mine, lines[j], 0.0), axis=0, keepdims=True)
            out_ref[j : j + 1, :] = line.astype(BF16)

    return pl.pallas_call(
        body,
        out_shape=jax.ShapeDtypeStruct((seqs, width), BF16),
        in_specs=[vmem()] * 2,
        out_specs=vmem(),
        compiler_params=SMALL,
    )(everyone, targets)


def per_device(q_nope, q_rope, latent_cache, rope_keys, lengths, slot_of, w_uk, w_uv, w_out):
    seqs = q_nope.shape[0]
    heads, nope_dim, _ = w_uk.shape
    scale = 1.0 / math.sqrt(nope_dim + q_rope.shape[1] // heads)
    seq_total = slot_of.shape[0]
    ranks = lax.axis_size("rank")
    z_groups, x_groups, c_groups = dp_groups()

    dp_pos = lax.axis_index("dp")
    plane_rows = 2 * NX * seqs
    at = jnp.arange(plane_rows, dtype=jnp.int32)
    from_c = (dp_pos % NC + at // (NX * seqs)) % NC
    place = at // seqs % NX
    step = jnp.where(place == 0, 0, (place + 1) % (NX - 1) + 1)
    from_x = (dp_pos // NC % NX + NX - step) % NX
    row_of = ((dp_pos // (NC * NX) * NX + from_x) * NC + from_c) * seqs + at % seqs
    slot_here = jnp.sum(
        jnp.where(
            row_of[:, None] == jnp.arange(seq_total, dtype=jnp.int32)[None, :], slot_of[None, :], 0
        ),
        axis=1,
    ).reshape(1, plane_rows)

    targets = lax.dynamic_slice_in_dim(slot_of, dp_pos * seqs, seqs).reshape(seqs, 1)

    sizes = [n for n in SIZES if n < seqs * latent_cache.shape[1]] + [seqs * latent_cache.shape[1]]
    needed = jnp.sum((lengths + BLOCK - 1) // BLOCK) * BLOCK
    which = sum((needed > n).astype(jnp.int32) for n in sizes[:-1])

    rows = join(q_nope, q_rope)
    near = [rows] + [shifted(rows, "dp", x_groups, k) for k in range(1, NX)]
    near = jnp.concatenate(placed_as(LAST_FAR, near), axis=0)
    far = shifted(near, "dp", c_groups, 1)
    picked = pick_rows(near, far, slot_here, seqs, (targets, which.reshape(1, 1)))
    arrived = lax.all_to_all(picked, "dp", 0, 0, axis_index_groups=z_groups, tiled=True)

    query_lat, query_rope = absorb(arrived, fetch(picked, w_uk), rope_keys.shape[1])

    def attend(packed):
        def branch(query_lat, query_rope, lengths, latent_cache, rope_keys, w_uv):
            own, *others, bounds, held = partial_scores(
                query_lat, query_rope, lengths, latent_cache, rope_keys, packed, scale
            )
            parts = placed_as(FIRST_FAR, [own] + from_ranks(others))
            weights = softmax(parts, bounds, seqs)
            gathered = [weights] + from_ranks([weights] * (ranks - 1))
            return head_part(gathered, bounds, held, w_uv, packed, seqs)

        return branch

    value_part = lax.switch(
        which,
        [attend(n) for n in sizes],
        query_lat,
        query_rope,
        lengths,
        latent_cache,
        rope_keys,
        w_uv,
    )
    parts = [value_part] + from_ranks([value_part] * (ranks - 1))
    copies = project(placed_as(LAST_FAR, parts), w_out, lax.axis_size("dp"))
    everyone = lax.all_to_all(copies, "dp", 0, 0, tiled=True)
    return bring_back(everyone, targets)


def solution(mesh):
    placed = (
        P("dp", None),
        P("dp", None),
        P("dp", None, "rank"),
        P("dp", "rank", None),
        P("dp"),
        P(),
        P(None, None, "rank"),
        P(None, "rank", None),
        P(None, "rank"),
    )
    return jax.shard_map(
        per_device, mesh=mesh, in_specs=placed, out_specs=P("dp", "rank"), check_vma=False
    )
```
